32 devices in a mesh: grid: 8 (over y, x, core), atom: 4 (over z).
Axes of the slice: x: 2, y: 2, z: 4, core: 2. Of those that a mesh axis runs over, the one named last changes fastest.
Arguments:
- basis_values: bfloat16 [64, 128, 512], P(('grid', 'atom')), may hold values from -8 to 8
- block_lists: int32 [64, 4], P('grid'), may hold values from 0 to 95, as said below
- orbitals: bfloat16 [12288, 4096], P('grid', 'atom'), may hold values from -0.00390625 to 0.00390625
- point_weights: float32 [8192], P(('grid', 'atom')), may hold values from 0.1 to 1
- point_atoms: int32 [8192], P(('grid', 'atom')), may hold values from 0 to 127, as said below
- embed_scale: float32 [256], replicated, may hold values from -4 to 4
- embed_shift: float32 [256], replicated, may hold values from -3 to 3
- message_weight: bfloat16 [2, 256, 256], replicated, may hold values from -0.375 to 0.375
- atom_weight: bfloat16 [2, 256, 256], replicated, may hold values from -0.375 to 0.375
- head_weight: float32 [256], replicated, may hold values from -0.375 to 0.375
Outputs:
- fock_orbitals: float32 [12288, 4096], P('grid', 'atom')
- potential: float32 [8192], P(('grid', 'atom'))
The draws below stay inside these ranges and needn't reach their ends.
Inputs may be any that keep to these rules, and one draw needn't show every extreme that they name: `block_lists`: each row names 4 different blocks; a batch b of group g = b // 8 names only blocks (g - 1) * 12 to (g + 2) * 12 - 1. `point_atoms`: the 256 points of one device name atom centres of one run of max(8, 1) consecutive centres, counted round.
All inputs are finite; a program needn't handle non-finite values.
Results may differ from the reference program's by a relative error of at most 0.04.
Values may be sent and summed in bfloat16 or wider, within the bound.
A program may use at most 128 MiB of HBM per device.

```python
import math
import jax
import jax.numpy as jnp
from jax import lax

BLK = 128
NBLK = 96
NLIST = 4
BPTS = 128
NOCC = 4096
FEAT = 256
LAYERS = 2
PT_DEV = 256
ATOM_DEV = 32
NB = 12288
NATOM = 128
POINTS = 8192
NBATCH = 64
N_GRID = 8


def draw_basis_values(key, part):
    owners = POINTS // PT_DEV
    per_owner = PT_DEV // BPTS
    key_scale = jax.random.fold_in(key, 21)
    key_entry = jax.random.fold_in(key, 22)
    exponent = jax.random.uniform(key_scale, (owners,), jnp.float32, -2.0, 1.5)
    owner_scale = jnp.repeat(jnp.exp(exponent), per_owner, total_repeat_length=NBATCH)
    entries = jax.random.normal(key_entry, (NBATCH, BPTS, NLIST * BLK), jnp.float32)
    batch_scale = jnp.ones((NBATCH,), jnp.float32)
    values = entries * (owner_scale * batch_scale)[:, None, None]
    return jnp.clip(values, -8.0, 8.0).astype(jnp.bfloat16)


def draw_block_lists(key, part):
    per_group = NBATCH // N_GRID
    owned = NBLK // N_GRID
    span = 3 * owned
    group = jnp.arange(NBATCH, dtype=jnp.int32) // per_group
    base = (group - 1) * owned
    offsets = jnp.arange(span, dtype=jnp.int32)
    positions = base[:, None] + offsets[None, :]
    outside = jnp.logical_or(positions < 0, positions >= NBLK).astype(jnp.int32)
    scores = jax.random.randint(key, (NBATCH, span), 0, 1048576, dtype=jnp.int32) * span + offsets[None, :]
    scores = scores + outside * 67108864
    order = jnp.argsort(scores, axis=1, stable=True).astype(jnp.int32)
    return base[:, None] + order[:, :NLIST]


def draw_point_atoms(key, part):
    key_start = jax.random.fold_in(key, 11)
    key_first = jax.random.fold_in(key, 12)
    key_second = jax.random.fold_in(key, 13)
    owners = POINTS // PT_DEV
    window = max(ATOM_DEV // 4, 1)
    starts = jax.random.randint(key_start, (owners,), 0, NATOM, dtype=jnp.int32)
    first = jax.random.randint(key_first, (owners, PT_DEV), 0, window, dtype=jnp.int32)
    second = jax.random.randint(key_second, (owners, PT_DEV), 0, window, dtype=jnp.int32)
    picked = jnp.minimum(first, second)
    return ((starts[:, None] + picked) % NATOM).reshape(-1).astype(jnp.int32)


def steps_of(own_key, shape, split, low, high):
    factor_of, own = 1.0, jax.random.fold_in(own_key, 6)
    for position, shards_of in split:
        heights = jnp.exp(jax.random.uniform(jax.random.fold_in(own, position), (shards_of,), jnp.float32, low / len(split), high / len(split)))
        factor_of = factor_of * jnp.repeat(heights, shape[position] // shards_of).reshape([-1 if axis == position else 1 for axis in range(len(shape))])
    return factor_of


def gaussian(own_key, dims, scale, most, shards=(), kind=jnp.bfloat16):
    result = jax.random.normal(own_key, dims, jnp.float32) * scale
    if len(shards) > 0:
        result = steps_of(own_key, dims, shards, -0.22, 0.18) * result
    return jnp.clip(result, min=-most, max=most).astype(kind)


def setup_inputs(seed: int = 0) -> dict:
    keys = jax.random.split(jax.random.key(seed), 11)
    return {
        "basis_values": draw_basis_values(jax.random.fold_in(keys[10], 71), 0),
        "block_lists": draw_block_lists(jax.random.fold_in(keys[10], 71), 0),
        "orbitals": gaussian(keys[2], (NB, NOCC), (NLIST * BLK * NOCC) ** -0.5, 0.00390625, ((0, 8), (1, 4))),
        "point_weights": jnp.clip(jnp.exp(math.log(1.0) - 2.3025851 * jax.random.uniform(keys[3], (POINTS,), jnp.float32) ** steps_of(keys[3], (POINTS,), ((0, 32),), -0.2, 0.2)), 0.1, 1.0),
        "point_atoms": draw_point_atoms(jax.random.fold_in(keys[10], 71), 0),
        "embed_scale": gaussian(keys[5], (FEAT,), 1.0, 4.0, (), jnp.float32),
        "embed_shift": gaussian(keys[6], (FEAT,), 0.7, 3.0, (), jnp.float32),
        "message_weight": gaussian(keys[7], (LAYERS, FEAT, FEAT), FEAT ** -0.5, 0.375),
        "atom_weight": gaussian(keys[8], (LAYERS, FEAT, FEAT), FEAT ** -0.5, 0.375),
        "head_weight": gaussian(keys[9], (FEAT,), FEAT ** -0.5, 0.375, (), jnp.float32),
    }


def orbital_values(values, lists, orbitals):
    blocks = orbitals.reshape(NBLK, BLK, NOCC)
    chosen = blocks[lists].reshape(lists.shape[0], NLIST * BLK, NOCC)
    psi = jnp.einsum("bpk,bko->bpo", values.astype(jnp.float32), chosen.astype(jnp.float32))
    return psi.astype(jnp.bfloat16)


def reference(basis_values, block_lists, orbitals, point_weights, point_atoms, embed_scale, embed_shift, message_weight, atom_weight, head_weight):
    grouped_values = basis_values.reshape(N_GRID, -1, BPTS, NLIST * BLK)
    grouped_lists = block_lists.reshape(N_GRID, -1, NLIST)

    def group_density(items):
        psi = orbital_values(items[0], items[1], orbitals)
        return 2.0 * jnp.sum(jnp.square(psi.astype(jnp.float32)), axis=2)

    density = lax.map(group_density, (grouped_values, grouped_lists)).reshape(-1)
    radius = jnp.cbrt(density)
    hidden = jax.nn.silu(radius[:, None] * embed_scale[None, :] + embed_shift[None, :])
    mass = jax.ops.segment_sum(point_weights, point_atoms, num_segments=NATOM)
    for layer in range(LAYERS):
        message = jax.nn.silu(jnp.dot(hidden.astype(jnp.bfloat16), message_weight[layer], preferred_element_type=jnp.float32))
        weighted = (point_weights[:, None] * message).astype(jnp.bfloat16)
        rows = jax.ops.segment_sum(weighted.astype(jnp.float32), point_atoms, num_segments=NATOM)
        mean = rows / (1.0 + mass[:, None])
        update = jax.nn.silu(jnp.dot(mean.astype(jnp.bfloat16), atom_weight[layer], preferred_element_type=jnp.float32)).astype(jnp.bfloat16)
        hidden = hidden + message * update[point_atoms].astype(jnp.float32)
    score = jnp.dot(hidden, head_weight, precision=lax.Precision.HIGHEST)
    potential = radius * (1.0 + jnp.tanh(score))
    scaled = (point_weights * potential).reshape(N_GRID, -1, BPTS)

    def group_fock(total, items):
        values, lists, scale = items
        psi = orbital_values(values, lists, orbitals)
        weighted_psi = (scale[:, :, None] * psi.astype(jnp.float32)).astype(jnp.bfloat16)
        terms = jnp.einsum("bpk,bpo->bko", values.astype(jnp.float32), weighted_psi.astype(jnp.float32))
        terms = terms.reshape(-1, BLK, NOCC)
        partial_value = jnp.zeros((NBLK, BLK, NOCC), jnp.float32).at[lists.reshape(-1)].add(terms)
        rounded = lax.optimization_barrier(partial_value.astype(jnp.bfloat16)).astype(jnp.float32)
        return total + rounded, None

    start = jnp.zeros((NBLK, BLK, NOCC), jnp.float32)
    total, unused = lax.scan(group_fock, start, (grouped_values, grouped_lists, scaled))
    return total.reshape(NB, NOCC), potential
```

```python
import functools
import jax
import jax.numpy as jnp
from jax import lax
from jax.experimental import pallas as pl
from jax.experimental.pallas import tpu as pltpu
from jax.sharding import PartitionSpec as P

ATOM_DEV = 32
RUN = max(ATOM_DEV // 4, 1)
LANES = 128
VMEM = pl.BlockSpec(memory_space=pltpu.VMEM)
MESH = pl.DeviceIdType.MESH


def passed_along(value, axis, steps):
    count = lax.axis_size(axis)
    leading, last = (max(0, -steps), min(count, count - steps))
    return lax.ppermute(value, axis, [(source, source + steps) for source in range(leading, last)])


def to_columns(rows):
    parts = [
        jnp.transpose(jnp.broadcast_to(rows[i : i + 1, :], (LANES, LANES)))
        for i in range(rows.shape[0])
    ]
    return jnp.concatenate(parts, axis=0)


def to_rows(columns):
    parts = []
    for i in range(columns.shape[0] // LANES):
        piece = jnp.broadcast_to(columns[i * LANES : (i + 1) * LANES, :], (LANES, LANES))
        parts.append(jnp.transpose(piece)[0:1, :])
    return jnp.concatenate(parts, axis=0)


def psi_kernel(lists, basis, below, own, above, psi, dens, rows, sums):
    step = pl.program_id(0)
    owned = own.shape[0]
    rows[0:owned, :] = below[...]
    rows[owned : 2 * owned, :] = own[...]
    rows[2 * owned : 3 * owned, :] = above[...]
    count, points, depth = basis.shape
    picks = lists.shape[1]
    width = depth // picks
    wide = psi.shape[2]

    @pl.when(step == 0)
    def _():
        sums[...] = jnp.zeros_like(sums)

    @pl.loop(0, count)
    def _(b):
        chosen = jnp.concatenate(
            [
                rows[pl.ds(pl.multiple_of(lists[b, j] * width, width), width), :]
                for j in range(picks)
            ],
            axis=0,
        )
        value = jnp.dot(basis[b], chosen, preferred_element_type=jnp.float32)
        rounded = value.astype(jnp.bfloat16)
        psi[b] = rounded
        square = jnp.square(rounded.astype(jnp.float32))
        total = square[:, 0:LANES]
        for i in range(1, wide // LANES):
            total = total + square[:, i * LANES : (i + 1) * LANES]
        sums[b] += total

    @pl.when(step == pl.num_programs(0) - 1)
    def _():
        for b in range(count):
            dens[b : b + 1, :] = jnp.sum(jnp.transpose(sums[b]), axis=0, keepdims=True)


def psi_and_density(lists, basis, below, own, above):
    owned, columns = own.shape
    count, points, depth = basis.shape
    wide = min(columns, 256)
    tile = pl.BlockSpec((owned, wide), lambda i, lists: (0, i))
    return pl.pallas_call(
        psi_kernel,
        out_shape=(
            jax.ShapeDtypeStruct((count, points, columns), jnp.bfloat16),
            jax.ShapeDtypeStruct((count, points), jnp.float32),
        ),
        grid_spec=pltpu.PrefetchScalarGridSpec(
            num_scalar_prefetch=1,
            grid=(columns // wide,),
            in_specs=[
                pl.BlockSpec((count, points, depth), lambda i, lists: (0, 0, 0)),
                tile,
                tile,
                tile,
            ],
            out_specs=(
                pl.BlockSpec((count, points, wide), lambda i, lists: (0, 0, i)),
                pl.BlockSpec((count, points), lambda i, lists: (0, 0)),
            ),
            scratch_shapes=[
                pltpu.VMEM((3 * owned, wide), jnp.bfloat16),
                pltpu.VMEM((count, points, LANES), jnp.float32),
            ],
        ),
        compiler_params=pltpu.CompilerParams(vmem_limit_bytes=48 << 20),
        cost_estimate=pl.CostEstimate(
            flops=2 * count * points * depth * columns,
            bytes_accessed=8 * owned * columns,
            transcendentals=0,
        ),
        name="psi_and_density",
    )(lists, basis, below, own, above)


def potential_kernel(
    shape, layers, dens, info, mine, hot, hot_t, weights, scale, shift, mw, aw, head,
    pot, near, dens_buf, info_buf, rows_out, rows_buf, scaled_out, scaled_buf, sent, got,
):
    n_grid, n_atom = shape
    n = n_grid * n_atom
    grid, atom = lax.axis_index("grid"), lax.axis_index("atom")
    me = grid * n_atom + atom

    def other(d):
        t = lax.rem(me + d, n)
        return (t // n_atom, lax.rem(t, n_atom))

    def to_all(source, held, k):
        @pl.loop(1, n)
        def _(d):
            pltpu.make_async_remote_copy(
                src_ref=source,
                dst_ref=held.at[me],
                send_sem=sent.at[k],
                recv_sem=got.at[k],
                device_id=other(d),
                device_id_type=MESH,
            ).start()

    def wait_all(held, sem, count):
        part = held.at[pl.ds(0, count)]
        pltpu.make_async_copy(part, part, sem).wait()

    barrier = pltpu.get_barrier_semaphore()

    @pl.loop(1, n)
    def _(d):
        pl.semaphore_signal(barrier, inc=1, device_id=other(d), device_id_type=MESH)

    pl.semaphore_wait(barrier, n - 1)

    @pl.loop(1, n_atom)
    def _(d):
        to = lax.rem(atom + d, n_atom)
        pltpu.make_async_remote_copy(
            src_ref=dens.at[to],
            dst_ref=dens_buf.at[atom],
            send_sem=sent.at[0],
            recv_sem=got.at[0],
            device_id=(grid, to),
            device_id_type=MESH,
        ).start()

    to_all(info, info_buf, 1)
    dens_buf[atom] = dens[atom]
    info_buf[me] = info[...]
    weight = to_columns(weights[...])[:, 0:1]

    wait_all(dens_buf, got.at[0], n_atom - 1)
    density = to_columns(2.0 * jnp.sum(dens_buf[...], axis=0))
    safe = jnp.where(density > 0.0, density, 1.0)
    radius = jnp.where(density > 0.0, jnp.exp(jnp.log(safe) * (1.0 / 3.0)), 0.0)[:, 0:1]
    hidden = jax.nn.silu(radius * scale[...] + shift[...])
    halves = hidden.shape[1] // LANES
    picks = []
    share = None
    for layer in range(layers):
        message = jax.nn.silu(
            jnp.dot(hidden.astype(jnp.bfloat16), mw[layer], preferred_element_type=jnp.float32)
        )
        weighted = (weight * message).astype(jnp.bfloat16)
        part = jnp.dot(hot_t[...], weighted, preferred_element_type=jnp.float32)
        rows_out[layer] = jnp.concatenate(
            [part[0:RUN, h * LANES : (h + 1) * LANES] for h in range(halves)], axis=0
        ).astype(jnp.bfloat16)
        to_all(rows_out.at[layer], rows_buf.at[layer], 2 + layer)
        rows_buf[layer, me] = rows_out[layer]
        if layer == 0:
            wait_all(info_buf, got.at[1], n - 1)
            facts = info_buf[...].reshape(n * RUN, LANES)
            same = (facts[:, 0:1] == mine[...]).astype(jnp.float32)
            mass = jnp.sum(same * facts[:, LANES // 2 : LANES // 2 + 1], axis=0, keepdims=True)
            share = 1.0 / (1.0 + to_columns(mass)[:, 0:1])
            same = same.reshape(n, RUN, LANES)
            none = jnp.zeros_like(same)
            for h in range(halves):
                full = jnp.concatenate(
                    [same if k == h else none for k in range(halves)], axis=1
                ).reshape(n * RUN * halves, LANES)
                picks.append(jnp.transpose(full).astype(jnp.bfloat16))
        wait_all(rows_buf.at[layer], got.at[2 + layer], n - 1)
        held = rows_buf[layer].reshape(n * RUN * halves, LANES)
        rows = jnp.concatenate(
            [jnp.dot(pick, held, preferred_element_type=jnp.float32) for pick in picks], axis=1
        )
        update = jax.nn.silu(
            jnp.dot(
                (rows * share).astype(jnp.bfloat16), aw[layer], preferred_element_type=jnp.float32
            )
        ).astype(jnp.bfloat16)
        picked = jnp.dot(hot[...], update, preferred_element_type=jnp.float32)
        hidden = hidden + message * picked
    score = jnp.sum(hidden * head[...], axis=1, keepdims=True)
    potential = radius * (1.0 + jnp.tanh(score))
    pot[...] = to_rows(potential)
    last = 2 + layers
    scaled_out[...] = to_rows(weight * potential)
    to_all(scaled_out, scaled_buf, last)
    scaled_buf[me] = scaled_out[...]
    wait_all(scaled_buf, got.at[last], n - 1)
    for k in range(3):
        group = jnp.clip(grid - 1 + k, 0, n_grid - 1)
        near[k * n_atom : (k + 1) * n_atom] = scaled_buf[pl.ds(group * n_atom, n_atom)]
    wait_all(dens_buf, sent.at[0], n_atom - 1)
    wait_all(info_buf, sent.at[1], n - 1)
    for layer in range(layers):
        wait_all(rows_buf.at[layer], sent.at[2 + layer], n - 1)
    wait_all(scaled_buf, sent.at[last], n - 1)


def potential_of(shape, dens, info, mine, hot, hot_t, weights, scale, shift, mw, aw, head):
    n_atom, batches, points = dens.shape
    n = shape[0] * shape[1]
    layers, features, _ = mw.shape
    packed = RUN * (features // LANES)
    return pl.pallas_call(
        functools.partial(potential_kernel, shape, layers),
        out_shape=(
            jax.ShapeDtypeStruct((batches, points), jnp.float32),
            jax.ShapeDtypeStruct((3 * n_atom, batches, points), jnp.float32),
        ),
        in_specs=[VMEM] * 11,
        out_specs=(VMEM, VMEM),
        scratch_shapes=[
            pltpu.VMEM((n_atom, batches, points), jnp.float32),
            pltpu.VMEM((n, RUN, LANES), jnp.float32),
            pltpu.VMEM((layers, packed, LANES), jnp.bfloat16),
            pltpu.VMEM((layers, n, packed, LANES), jnp.bfloat16),
            pltpu.VMEM((batches, points), jnp.float32),
            pltpu.VMEM((n, batches, points), jnp.float32),
            pltpu.SemaphoreType.DMA((3 + layers,)),
            pltpu.SemaphoreType.DMA((3 + layers,)),
        ],
        compiler_params=pltpu.CompilerParams(
            collective_id=0, has_side_effects=True, vmem_limit_bytes=32 << 20
        ),
        cost_estimate=pl.CostEstimate(
            flops=20_000_000_000, bytes_accessed=4_000_000, transcendentals=0
        ),
        name="potential_of",
    )(dens, info, mine, hot, hot_t, weights, scale, shift, mw, aw, head)


def fock_kernel(lists, basis_t, near, low, mid, high, out, scaled):
    step = pl.program_id(0)
    groups, count, depth, points = basis_t.shape
    picks = lists.shape[1]
    width = depth // picks
    owned = out.shape[0] // width

    @pl.when(step == 0)
    def _():
        @pl.loop(0, groups)
        def _(k):
            @pl.loop(0, count)
            def _(b):
                scaled[k, b] = (
                    basis_t[k, b].astype(jnp.float32) * near[pl.ds(k * count + b, 1), :]
                ).astype(jnp.bfloat16)

    out[...] = jnp.zeros_like(out)
    for k, psi in enumerate((low, mid, high)):

        @pl.loop(0, count)
        def _(b, k=k, psi=psi):
            for j in range(picks):
                block = lists[k * count + b, j]

                @pl.when(jnp.logical_and(block >= 0, block < owned))
                def _():
                    at = pl.ds(pl.multiple_of(block * width, width), width)
                    out[at, :] += jnp.dot(
                        scaled[k, b, j * width : (j + 1) * width, :],
                        psi[b],
                        preferred_element_type=jnp.float32,
                    )


def fock_of(lists, basis_t, near, low, mid, high, owned):
    groups, count, depth, points = basis_t.shape
    columns = mid.shape[2]
    wide = min(columns, 512)
    tile = pl.BlockSpec((count, points, wide), lambda i, lists: (0, 0, i))
    return pl.pallas_call(
        fock_kernel,
        out_shape=jax.ShapeDtypeStruct((owned, columns), jnp.float32),
        grid_spec=pltpu.PrefetchScalarGridSpec(
            num_scalar_prefetch=1,
            grid=(columns // wide,),
            in_specs=[
                pl.BlockSpec((groups, count, depth, points), lambda i, lists: (0, 0, 0, 0)),
                pl.BlockSpec((groups * count, points), lambda i, lists: (0, 0)),
                tile,
                tile,
                tile,
            ],
            out_specs=pl.BlockSpec((owned, wide), lambda i, lists: (0, i)),
            scratch_shapes=[pltpu.VMEM((groups, count, depth, points), jnp.bfloat16)],
        ),
        compiler_params=pltpu.CompilerParams(vmem_limit_bytes=60 << 20),
        name="fock_of",
    )(lists, basis_t, near, low, mid, high)


def local(
    basis_values,
    block_lists,
    orbitals,
    point_weights,
    point_atoms,
    embed_scale,
    embed_shift,
    message_weight,
    atom_weight,
    head_weight,
):
    n_grid, n_atom = lax.axis_size("grid"), lax.axis_size("atom")
    own_rows = orbitals.shape[0]
    batches, points, depth = basis_values.shape
    width = depth // block_lists.shape[1]
    owned = own_rows // width
    below = passed_along(orbitals, "grid", 1)
    above = passed_along(orbitals, "grid", -1)
    values = lax.all_gather(basis_values, "atom", axis=0, tiled=True)
    piece_t = jnp.swapaxes(basis_values, 1, 2)
    beside = jnp.stack([passed_along(piece_t, "grid", 1), passed_along(piece_t, "grid", -1)])
    beside = lax.all_gather(beside, "atom", axis=1, tiled=True)
    basis_t = jnp.stack([beside[0], jnp.swapaxes(values, 1, 2), beside[1]])
    first = lax.axis_index("grid") * owned
    lists_low = passed_along(block_lists + 1, "grid", 1) - 1
    lists_high = passed_along(block_lists + 1, "grid", -1) - 1
    lists = jnp.concatenate([lists_low, block_lists, lists_high], axis=0) - first

    total = ATOM_DEV * n_atom
    lead = point_atoms[0]
    shifted = (point_atoms - lead + total // 2) % total - total // 2
    least = jnp.min(shifted)
    start = (lead + least) % total
    place = shifted - least
    lanes = jnp.arange(LANES, dtype=jnp.int32)
    onehot = place[:, None] == lanes[None, :]
    hot = onehot.astype(jnp.bfloat16)
    hot_t = (place[None, :] == lanes[:, None]).astype(jnp.bfloat16)
    mass = jnp.sum(jnp.where(onehot, point_weights[:, None], 0.0), axis=0)[:RUN]
    names = ((start + lanes) % total).astype(jnp.float32)
    mine = jnp.where(lanes < RUN, names, -1.0)[None, :]
    info = jnp.where(lanes[None, :] < LANES // 2, names[:RUN, None], mass[:, None])

    psi, dens = psi_and_density(block_lists - first + owned, values, below, orbitals, above)
    psi_low = passed_along(psi, "grid", 1)
    psi_high = passed_along(psi, "grid", -1)
    potential, near = potential_of(
        (n_grid, n_atom),
        dens.reshape(n_atom, batches, points),
        info,
        mine,
        hot,
        hot_t,
        point_weights.reshape(batches, points),
        embed_scale[None, :],
        embed_shift[None, :],
        message_weight,
        atom_weight,
        head_weight[None, :],
    )
    fock = fock_of(
        lists, basis_t, near.reshape(-1, points), psi_low, psi, psi_high, own_rows
    )
    return (fock, potential.reshape(-1))


def solution(mesh):
    return jax.shard_map(
        local,
        mesh=mesh,
        in_specs=(
            P(("grid", "atom"), None, None),
            P("grid", None),
            P("grid", "atom"),
            P(("grid", "atom")),
            P(("grid", "atom")),
            P(),
            P(),
            P(),
            P(),
            P(),
        ),
        out_specs=(P("grid", "atom"), P(("grid", "atom"))),
        check_vma=False,
    )
```

```python
import functools
import jax
import jax.numpy as jnp
from jax import lax
from jax.experimental import pallas as pl
from jax.experimental.pallas import tpu as pltpu
from jax.sharding import PartitionSpec as P

ATOM_DEV = 32
RUN = max(ATOM_DEV // 4, 1)
LANES = 128
VMEM = pl.BlockSpec(memory_space=pltpu.VMEM)
MESH = pl.DeviceIdType.MESH


def wait_bytes(ref, sem):
    pltpu.make_async_copy(ref, ref, sem).wait()


class Halo:
    def __init__(self, n_grid, rounds, source, low, high, relay, sent, got, passed):
        self.n_grid, self.rounds, self.middle = n_grid, rounds, n_grid // 2
        self.source, self.low, self.high, self.relay = source, low, high, relay
        self.sent, self.got, self.passed = sent, got, passed
        self.size = source.shape[0] // (2 * rounds)
        self.grid, self.atom = lax.axis_index("grid"), lax.axis_index("atom")

    def copy(self, source, target, sent, got, grid):
        pltpu.make_async_remote_copy(
            src_ref=source,
            dst_ref=target,
            send_sem=sent,
            recv_sem=got,
            device_id=(grid, self.atom),
            device_id_type=MESH,
        ).start()

    def send(self, r):
        grid, last, size = self.grid, self.n_grid - 1, self.size
        for way, (step, held, split, able) in enumerate(
            (
                (1, self.low, self.middle - 1, grid < last),
                (-1, self.high, self.middle, grid > 0),
            )
        ):
            for side, end in enumerate((0, last)):
                part = pl.ds((side * self.rounds + r) * size, size)

                @pl.when(jnp.logical_and(able, grid != split))
                def _():
                    self.copy(
                        self.source.at[part], held.at[part],
                        self.sent.at[way], self.got.at[way], grid + step,
                    )

                @pl.when(grid == split)
                def _():
                    self.copy(
                        self.source.at[part], self.relay.at[way, pl.ds(r * size, size)],
                        self.sent.at[way], self.passed.at[way, r], end,
                    )

    def forward(self, r):
        size = self.size
        for side, end in enumerate((0, self.n_grid - 1)):

            @pl.when(self.grid == end)
            def _():
                for way, (held, to) in enumerate(
                    ((self.low, self.middle), (self.high, self.middle - 1))
                ):
                    piece = self.relay.at[way, pl.ds(r * size, size)]
                    wait_bytes(piece, self.passed.at[way, r])
                    part = pl.ds((side * self.rounds + r) * size, size)
                    self.copy(piece, held.at[part], self.sent.at[2 + way], self.got.at[way], to)

    def finish(self):
        grid, last = self.grid, self.n_grid - 1

        @pl.when(grid > 0)
        def _():
            wait_bytes(self.low, self.got.at[0])
            wait_bytes(self.source, self.sent.at[1])

        @pl.when(grid < last)
        def _():
            wait_bytes(self.high, self.got.at[1])
            wait_bytes(self.source, self.sent.at[0])

        @pl.when(jnp.logical_or(grid == 0, grid == last))
        def _():
            for way in range(2):
                wait_bytes(self.relay.at[way], self.sent.at[2 + way])


def halo_scratch(rounds):
    return [
        pltpu.SemaphoreType.DMA((4,)),
        pltpu.SemaphoreType.DMA((2,)),
        pltpu.SemaphoreType.DMA((2, rounds)),
    ]


def meet_all(shape):
    n_grid, n_atom = shape
    n = n_grid * n_atom
    me = lax.axis_index("grid") * n_atom + lax.axis_index("atom")
    barrier = pltpu.get_barrier_semaphore()

    @pl.loop(1, n)
    def _(d):
        t = lax.rem(me + d, n)
        pl.semaphore_signal(
            barrier, inc=1, device_id=(t // n_atom, lax.rem(t, n_atom)), device_id_type=MESH
        )

    pl.semaphore_wait(barrier, n - 1)


ROUNDS = 4


def halo_kernel(
    shape, own, piece, names, low, high, basis, all_names, relay,
    sent, got, passed, piece_sent, piece_got, name_sent, name_got,
):
    n_grid, n_atom = shape
    grid, atom = lax.axis_index("grid"), lax.axis_index("atom")
    meet_all(shape)
    halo = Halo(n_grid, ROUNDS, own, low, high, relay, sent, got, passed)

    def send(source, target, sent_sem, got_sem, to):
        pltpu.make_async_remote_copy(
            src_ref=source,
            dst_ref=target,
            send_sem=sent_sem,
            recv_sem=got_sem,
            device_id=to,
            device_id_type=MESH,
        ).start()

    sides = ((0, 1, grid < n_grid - 1, grid > 0), (2, -1, grid > 0, grid < n_grid - 1))
    for slot, step, able, _ in sides:

        @pl.when(able)
        def _():
            send(names, all_names.at[slot], name_sent.at[slot], name_got.at[slot], (grid + step, atom))
            send(piece, basis.at[slot, atom], piece_sent.at[slot], piece_got.at[slot], (grid + step, atom))

    def to_peers(source, slot, k):
        @pl.loop(1, n_atom)
        def _(d):
            to = lax.rem(atom + d, n_atom)
            send(source, basis.at[slot, atom], piece_sent.at[k], piece_got.at[k], (grid, to))

    to_peers(piece, 1, 1)
    for r in range(ROUNDS):
        halo.send(r)
    basis[1, atom] = piece[...]
    all_names[1] = names[...]
    for slot, _, _, filled in sides:

        @pl.when(filled)
        def _():
            wait_bytes(piece, piece_got.at[slot])
            to_peers(basis.at[slot, atom], slot, 3 + slot // 2)

        @pl.when(jnp.logical_not(filled))
        def _():
            all_names[slot] = jnp.full_like(names, -1)

    for r in range(ROUNDS):
        halo.forward(r)
    peers = pl.ds(0, n_atom - 1)
    wait_bytes(basis.at[1, peers], piece_got.at[1])
    wait_bytes(basis.at[1, peers], piece_sent.at[1])
    for slot, _, able, filled in sides:

        @pl.when(able)
        def _():
            wait_bytes(piece, piece_sent.at[slot])
            wait_bytes(names, name_sent.at[slot])

        @pl.when(filled)
        def _():
            wait_bytes(names, name_got.at[slot])
            wait_bytes(basis.at[slot, peers], piece_got.at[3 + slot // 2])
            wait_bytes(basis.at[slot, peers], piece_sent.at[3 + slot // 2])

    halo.finish()


def halo_of(shape, own, piece, names):
    rows, columns = own.shape
    anywhere = pl.BlockSpec(memory_space=pl.ANY)
    return pl.pallas_call(
        functools.partial(halo_kernel, shape),
        out_shape=(
            jax.ShapeDtypeStruct(own.shape, own.dtype),
            jax.ShapeDtypeStruct(own.shape, own.dtype),
            jax.ShapeDtypeStruct((3, shape[1], *piece.shape), piece.dtype),
            jax.ShapeDtypeStruct((3, *names.shape), names.dtype),
            jax.ShapeDtypeStruct((2, rows // 2, columns), own.dtype),
        ),
        in_specs=[anywhere, VMEM, VMEM],
        out_specs=(anywhere, anywhere, VMEM, VMEM, anywhere),
        scratch_shapes=halo_scratch(ROUNDS)
        + [
            pltpu.SemaphoreType.DMA((5,)),
            pltpu.SemaphoreType.DMA((5,)),
            pltpu.SemaphoreType.DMA((3,)),
            pltpu.SemaphoreType.DMA((3,)),
        ],
        compiler_params=pltpu.CompilerParams(
            collective_id=1, has_side_effects=True, vmem_limit_bytes=40 << 20
        ),
        name="halo_of",
    )(own, piece, names)


def to_columns(rows):
    parts = [
        jnp.transpose(jnp.broadcast_to(rows[i : i + 1, :], (LANES, LANES)))
        for i in range(rows.shape[0])
    ]
    return jnp.concatenate(parts, axis=0)


def to_rows(columns):
    parts = []
    for i in range(columns.shape[0] // LANES):
        piece = jnp.broadcast_to(columns[i * LANES : (i + 1) * LANES, :], (LANES, LANES))
        parts.append(jnp.transpose(piece)[0:1, :])
    return jnp.concatenate(parts, axis=0)


def psi_kernel(lists, basis_t, below, own, above, psi, dens, rows, sums, basis):
    step = pl.program_id(0)
    owned = own.shape[0]
    rows[0:owned, :] = below[...]
    rows[owned : 2 * owned, :] = own[...]
    rows[2 * owned : 3 * owned, :] = above[...]
    count, points, depth = basis.shape
    picks = lists.shape[1]
    width = depth // picks
    wide = psi.shape[2]

    @pl.when(step == 0)
    def _():
        sums[...] = jnp.zeros_like(sums)
        for b in range(count):
            basis[b] = jnp.transpose(basis_t[0, b])

    @pl.loop(0, count)
    def _(b):
        chosen = jnp.concatenate(
            [
                rows[pl.ds(pl.multiple_of(lists[b, j] * width, width), width), :]
                for j in range(picks)
            ],
            axis=0,
        )
        value = jnp.dot(basis[b], chosen, preferred_element_type=jnp.float32)
        rounded = value.astype(jnp.bfloat16)
        psi[b] = rounded
        square = jnp.square(rounded.astype(jnp.float32))
        total = square[:, 0:LANES]
        for i in range(1, wide // LANES):
            total = total + square[:, i * LANES : (i + 1) * LANES]
        sums[b] += total

    @pl.when(step == pl.num_programs(0) - 1)
    def _():
        for b in range(count):
            dens[b : b + 1, :] = jnp.sum(jnp.transpose(sums[b]), axis=0, keepdims=True)


def psi_and_density(lists, basis_t, below, own, above):
    owned, columns = own.shape
    _, count, depth, points = basis_t.shape
    wide = min(columns, 256)
    tile = pl.BlockSpec((owned, wide), lambda i, lists: (0, i))
    return pl.pallas_call(
        psi_kernel,
        out_shape=(
            jax.ShapeDtypeStruct((count, points, columns), jnp.bfloat16),
            jax.ShapeDtypeStruct((count, points), jnp.float32),
        ),
        grid_spec=pltpu.PrefetchScalarGridSpec(
            num_scalar_prefetch=1,
            grid=(columns // wide,),
            in_specs=[
                pl.BlockSpec((1, count, depth, points), lambda i, lists: (1, 0, 0, 0)),
                tile,
                tile,
                tile,
            ],
            out_specs=(
                pl.BlockSpec((count, points, wide), lambda i, lists: (0, 0, i)),
                pl.BlockSpec((count, points), lambda i, lists: (0, 0)),
            ),
            scratch_shapes=[
                pltpu.VMEM((3 * owned, wide), jnp.bfloat16),
                pltpu.VMEM((count, points, LANES), jnp.float32),
                pltpu.VMEM((count, points, depth), jnp.bfloat16),
            ],
        ),
        compiler_params=pltpu.CompilerParams(vmem_limit_bytes=48 << 20),
        cost_estimate=pl.CostEstimate(
            flops=2 * count * points * depth * columns,
            bytes_accessed=8 * owned * columns,
            transcendentals=0,
        ),
        name="psi_and_density",
    )(lists, basis_t, below, own, above)


def potential_kernel(
    shape, layers, psi, dens, info, mine, hot, hot_t, weights, scale, shift, mw, aw, head,
    pot, near, psi_low, psi_high, relay,
    dens_buf, info_buf, rows_out, rows_buf, scaled_out, scaled_buf, sent, got,
    psi_sent, psi_got, psi_passed,
):
    n_grid, n_atom = shape
    n = n_grid * n_atom
    grid, atom = lax.axis_index("grid"), lax.axis_index("atom")
    me = grid * n_atom + atom

    def other(d):
        t = lax.rem(me + d, n)
        return (t // n_atom, lax.rem(t, n_atom))

    def to_all(source, held, k):
        @pl.loop(1, n)
        def _(d):
            pltpu.make_async_remote_copy(
                src_ref=source,
                dst_ref=held.at[me],
                send_sem=sent.at[k],
                recv_sem=got.at[k],
                device_id=other(d),
                device_id_type=MESH,
            ).start()

    def wait_all(held, sem, count):
        part = held.at[pl.ds(0, count)]
        pltpu.make_async_copy(part, part, sem).wait()

    meet_all(shape)
    halo = Halo(n_grid, layers + 2, psi, psi_low, psi_high, relay, psi_sent, psi_got, psi_passed)

    @pl.loop(1, n_atom)
    def _(d):
        to = lax.rem(atom + d, n_atom)
        pltpu.make_async_remote_copy(
            src_ref=dens.at[to],
            dst_ref=dens_buf.at[atom],
            send_sem=sent.at[0],
            recv_sem=got.at[0],
            device_id=(grid, to),
            device_id_type=MESH,
        ).start()

    to_all(info, info_buf, 1)
    halo.send(0)
    dens_buf[atom] = dens[atom]
    info_buf[me] = info[...]
    weight = to_columns(weights[...])[:, 0:1]

    wait_all(dens_buf, got.at[0], n_atom - 1)
    density = to_columns(2.0 * jnp.sum(dens_buf[...], axis=0))
    safe = jnp.where(density > 0.0, density, 1.0)
    radius = jnp.where(density > 0.0, jnp.exp(jnp.log(safe) * (1.0 / 3.0)), 0.0)[:, 0:1]
    hidden = jax.nn.silu(radius * scale[...] + shift[...])
    halves = hidden.shape[1] // LANES
    picks = []
    share = None
    for layer in range(layers):
        message = jax.nn.silu(
            jnp.dot(hidden.astype(jnp.bfloat16), mw[layer], preferred_element_type=jnp.float32)
        )
        weighted = (weight * message).astype(jnp.bfloat16)
        part = jnp.dot(hot_t[...], weighted, preferred_element_type=jnp.float32)
        rows_out[layer] = jnp.concatenate(
            [part[0:RUN, h * LANES : (h + 1) * LANES] for h in range(halves)], axis=0
        ).astype(jnp.bfloat16)
        to_all(rows_out.at[layer], rows_buf.at[layer], 2 + layer)
        halo.send(1 + layer)
        rows_buf[layer, me] = rows_out[layer]
        if layer == 0:
            wait_all(info_buf, got.at[1], n - 1)
            facts = info_buf[...].reshape(n * RUN, LANES)
            same = (facts[:, 0:1] == mine[...]).astype(jnp.float32)
            mass = jnp.sum(same * facts[:, LANES // 2 : LANES // 2 + 1], axis=0, keepdims=True)
            share = 1.0 / (1.0 + to_columns(mass)[:, 0:1])
            same = same.reshape(n, RUN, LANES)
            none = jnp.zeros_like(same)
            for h in range(halves):
                full = jnp.concatenate(
                    [same if k == h else none for k in range(halves)], axis=1
                ).reshape(n * RUN * halves, LANES)
                picks.append(jnp.transpose(full).astype(jnp.bfloat16))
        wait_all(rows_buf.at[layer], got.at[2 + layer], n - 1)
        halo.forward(layer)
        held = rows_buf[layer].reshape(n * RUN * halves, LANES)
        rows = jnp.concatenate(
            [jnp.dot(pick, held, preferred_element_type=jnp.float32) for pick in picks], axis=1
        )
        update = jax.nn.silu(
            jnp.dot(
                (rows * share).astype(jnp.bfloat16), aw[layer], preferred_element_type=jnp.float32
            )
        ).astype(jnp.bfloat16)
        picked = jnp.dot(hot[...], update, preferred_element_type=jnp.float32)
        hidden = hidden + message * picked
    score = jnp.sum(hidden * head[...], axis=1, keepdims=True)
    potential = radius * (1.0 + jnp.tanh(score))
    pot[...] = to_rows(potential)
    last = 2 + layers
    scaled_out[...] = to_rows(weight * potential)
    to_all(scaled_out, scaled_buf, last)
    halo.send(layers + 1)
    scaled_buf[me] = scaled_out[...]
    wait_all(scaled_buf, got.at[last], n - 1)
    halo.forward(layers)
    halo.forward(layers + 1)
    for k in range(3):
        group = jnp.clip(grid - 1 + k, 0, n_grid - 1)
        near[k * n_atom : (k + 1) * n_atom] = scaled_buf[pl.ds(group * n_atom, n_atom)]
    wait_all(dens_buf, sent.at[0], n_atom - 1)
    wait_all(info_buf, sent.at[1], n - 1)
    for layer in range(layers):
        wait_all(rows_buf.at[layer], sent.at[2 + layer], n - 1)
    wait_all(scaled_buf, sent.at[last], n - 1)
    halo.finish()


def potential_of(shape, psi, dens, info, mine, hot, hot_t, weights, scale, shift, mw, aw, head):
    n_atom, batches, points = dens.shape
    n = shape[0] * shape[1]
    layers, features, _ = mw.shape
    packed = RUN * (features // LANES)
    anywhere = pl.BlockSpec(memory_space=pl.ANY)
    return pl.pallas_call(
        functools.partial(potential_kernel, shape, layers),
        out_shape=(
            jax.ShapeDtypeStruct((batches, points), jnp.float32),
            jax.ShapeDtypeStruct((3 * n_atom, batches, points), jnp.float32),
            jax.ShapeDtypeStruct(psi.shape, psi.dtype),
            jax.ShapeDtypeStruct(psi.shape, psi.dtype),
            jax.ShapeDtypeStruct((2, psi.shape[0] // 2, *psi.shape[1:]), psi.dtype),
        ),
        in_specs=[anywhere] + [VMEM] * 11,
        out_specs=(VMEM, VMEM, anywhere, anywhere, anywhere),
        scratch_shapes=[
            pltpu.VMEM((n_atom, batches, points), jnp.float32),
            pltpu.VMEM((n, RUN, LANES), jnp.float32),
            pltpu.VMEM((layers, packed, LANES), jnp.bfloat16),
            pltpu.VMEM((layers, n, packed, LANES), jnp.bfloat16),
            pltpu.VMEM((batches, points), jnp.float32),
            pltpu.VMEM((n, batches, points), jnp.float32),
            pltpu.SemaphoreType.DMA((3 + layers,)),
            pltpu.SemaphoreType.DMA((3 + layers,)),
        ]
        + halo_scratch(layers + 2),
        compiler_params=pltpu.CompilerParams(
            collective_id=0, has_side_effects=True, vmem_limit_bytes=32 << 20
        ),
        cost_estimate=pl.CostEstimate(
            flops=20_000_000_000, bytes_accessed=4_000_000, transcendentals=0
        ),
        name="potential_of",
    )(psi, dens, info, mine, hot, hot_t, weights, scale, shift, mw, aw, head)


def fock_kernel(lists, basis_t, near, low, mid, high, out, scaled):
    step = pl.program_id(0)
    groups, count, depth, points = basis_t.shape
    picks = lists.shape[1]
    width = depth // picks
    owned = out.shape[0] // width

    @pl.when(step == 0)
    def _():
        @pl.loop(0, groups)
        def _(k):
            @pl.loop(0, count)
            def _(b):
                scaled[k, b] = (
                    basis_t[k, b].astype(jnp.float32) * near[pl.ds(k * count + b, 1), :]
                ).astype(jnp.bfloat16)

    out[...] = jnp.zeros_like(out)
    for k, psi in enumerate((low, mid, high)):

        @pl.loop(0, count)
        def _(b, k=k, psi=psi):
            for j in range(picks):
                block = lists[k * count + b, j]

                @pl.when(jnp.logical_and(block >= 0, block < owned))
                def _():
                    at = pl.ds(pl.multiple_of(block * width, width), width)
                    out[at, :] += jnp.dot(
                        scaled[k, b, j * width : (j + 1) * width, :],
                        psi[b],
                        preferred_element_type=jnp.float32,
                    )


def fock_of(lists, basis_t, near, low, mid, high, owned):
    groups, count, depth, points = basis_t.shape
    columns = mid.shape[2]
    wide = min(columns, 512)
    tile = pl.BlockSpec((count, points, wide), lambda i, lists: (0, 0, i))
    return pl.pallas_call(
        fock_kernel,
        out_shape=jax.ShapeDtypeStruct((owned, columns), jnp.float32),
        grid_spec=pltpu.PrefetchScalarGridSpec(
            num_scalar_prefetch=1,
            grid=(columns // wide,),
            in_specs=[
                pl.BlockSpec((groups, count, depth, points), lambda i, lists: (0, 0, 0, 0)),
                pl.BlockSpec((groups * count, points), lambda i, lists: (0, 0)),
                tile,
                tile,
                tile,
            ],
            out_specs=pl.BlockSpec((owned, wide), lambda i, lists: (0, i)),
            scratch_shapes=[pltpu.VMEM((groups, count, depth, points), jnp.bfloat16)],
        ),
        compiler_params=pltpu.CompilerParams(vmem_limit_bytes=60 << 20),
        name="fock_of",
    )(lists, basis_t, near, low, mid, high)


def local(
    basis_values,
    block_lists,
    orbitals,
    point_weights,
    point_atoms,
    embed_scale,
    embed_shift,
    message_weight,
    atom_weight,
    head_weight,
):
    n_grid, n_atom = lax.axis_size("grid"), lax.axis_size("atom")
    own_rows = orbitals.shape[0]
    batches, points, depth = basis_values.shape
    width = depth // block_lists.shape[1]
    owned = own_rows // width
    shape = (n_grid, n_atom)
    first = lax.axis_index("grid") * owned
    names = jnp.pad(block_lists, ((0, 0), (0, LANES - block_lists.shape[1])))
    below, above, basis_t, names, _ = halo_of(
        shape, orbitals, jnp.swapaxes(basis_values, 1, 2), names
    )
    basis_t = basis_t.reshape(3, n_atom * batches, depth, points)
    lists = names[:, :, : block_lists.shape[1]].reshape(-1, block_lists.shape[1]) - first

    total = ATOM_DEV * n_atom
    lead = point_atoms[0]
    shifted = (point_atoms - lead + total // 2) % total - total // 2
    least = jnp.min(shifted)
    start = (lead + least) % total
    place = shifted - least
    lanes = jnp.arange(LANES, dtype=jnp.int32)
    onehot = place[:, None] == lanes[None, :]
    hot = onehot.astype(jnp.bfloat16)
    hot_t = (place[None, :] == lanes[:, None]).astype(jnp.bfloat16)
    mass = jnp.sum(jnp.where(onehot, point_weights[:, None], 0.0), axis=0)[:RUN]
    names = ((start + lanes) % total).astype(jnp.float32)
    mine = jnp.where(lanes < RUN, names, -1.0)[None, :]
    info = jnp.where(lanes[None, :] < LANES // 2, names[:RUN, None], mass[:, None])

    psi, dens = psi_and_density(block_lists - first + owned, basis_t, below, orbitals, above)
    potential, near, psi_low, psi_high, _ = potential_of(
        shape,
        psi,
        dens.reshape(n_atom, batches, points),
        info,
        mine,
        hot,
        hot_t,
        point_weights.reshape(batches, points),
        embed_scale[None, :],
        embed_shift[None, :],
        message_weight,
        atom_weight,
        head_weight[None, :],
    )
    fock = fock_of(
        lists, basis_t, near.reshape(-1, points), psi_low, psi, psi_high, own_rows
    )
    return (fock, potential.reshape(-1))


def solution(mesh):
    return jax.shard_map(
        local,
        mesh=mesh,
        in_specs=(
            P(("grid", "atom"), None, None),
            P("grid", None),
            P("grid", "atom"),
            P(("grid", "atom")),
            P(("grid", "atom")),
            P(),
            P(),
            P(),
            P(),
            P(),
        ),
        out_specs=(P("grid", "atom"), P(("grid", "atom"))),
        check_vma=False,
    )
```

```python
import functools
import jax
import jax.numpy as jnp
from jax import lax
from jax.experimental import pallas as pl
from jax.experimental.pallas import tpu as pltpu
from jax.sharding import PartitionSpec as P

ATOM_DEV = 32
RUN = max(ATOM_DEV // 4, 1)
LANES = 128
VMEM = pl.BlockSpec(memory_space=pltpu.VMEM)
MESH = pl.DeviceIdType.MESH


def wait_bytes(ref, sem):
    pltpu.make_async_copy(ref, ref, sem).wait()


class Halo:
    def __init__(self, n_grid, rounds, source, low, high, relay, sent, got, passed):
        self.n_grid, self.rounds, self.middle = n_grid, rounds, n_grid // 2
        self.source, self.low, self.high, self.relay = source, low, high, relay
        self.sent, self.got, self.passed = sent, got, passed
        self.size = source.shape[0] // (2 * rounds)
        self.grid, self.atom = lax.axis_index("grid"), lax.axis_index("atom")

    def copy(self, source, target, sent, got, grid):
        pltpu.make_async_remote_copy(
            src_ref=source,
            dst_ref=target,
            send_sem=sent,
            recv_sem=got,
            device_id=(grid, self.atom),
            device_id_type=MESH,
        ).start()

    def send(self, r):
        grid, last, size = self.grid, self.n_grid - 1, self.size
        for way, (step, held, split, able) in enumerate(
            (
                (1, self.low, self.middle - 1, grid < last),
                (-1, self.high, self.middle, grid > 0),
            )
        ):
            for side, end in enumerate((0, last)):
                part = pl.ds((side * self.rounds + r) * size, size)

                @pl.when(jnp.logical_and(able, grid != split))
                def _():
                    self.copy(
                        self.source.at[part], held.at[part],
                        self.sent.at[way], self.got.at[way], grid + step,
                    )

                @pl.when(grid == split)
                def _():
                    self.copy(
                        self.source.at[part], self.relay.at[way, pl.ds(r * size, size)],
                        self.sent.at[way], self.passed.at[way, r], end,
                    )

    def forward(self, r):
        size = self.size
        for side, end in enumerate((0, self.n_grid - 1)):

            @pl.when(self.grid == end)
            def _():
                for way, (held, to) in enumerate(
                    ((self.low, self.middle), (self.high, self.middle - 1))
                ):
                    piece = self.relay.at[way, pl.ds(r * size, size)]
                    wait_bytes(piece, self.passed.at[way, r])
                    part = pl.ds((side * self.rounds + r) * size, size)
                    self.copy(piece, held.at[part], self.sent.at[2 + way], self.got.at[way], to)

    def finish(self):
        grid, last = self.grid, self.n_grid - 1

        @pl.when(grid > 0)
        def _():
            wait_bytes(self.low, self.got.at[0])
            wait_bytes(self.source, self.sent.at[1])

        @pl.when(grid < last)
        def _():
            wait_bytes(self.high, self.got.at[1])
            wait_bytes(self.source, self.sent.at[0])

        @pl.when(jnp.logical_or(grid == 0, grid == last))
        def _():
            for way in range(2):
                wait_bytes(self.relay.at[way], self.sent.at[2 + way])


def halo_scratch(rounds):
    return [
        pltpu.SemaphoreType.DMA((4,)),
        pltpu.SemaphoreType.DMA((2,)),
        pltpu.SemaphoreType.DMA((2, rounds)),
    ]


def meet_all(shape):
    n_grid, n_atom = shape
    n = n_grid * n_atom
    me = lax.axis_index("grid") * n_atom + lax.axis_index("atom")
    barrier = pltpu.get_barrier_semaphore()

    @pl.loop(1, n)
    def _(d):
        t = lax.rem(me + d, n)
        pl.semaphore_signal(
            barrier, inc=1, device_id=(t // n_atom, lax.rem(t, n_atom)), device_id_type=MESH
        )

    pl.semaphore_wait(barrier, n - 1)


ROUNDS = 4


def halo_kernel(
    shape, own, piece, names, low, high, basis, beside, all_names, relay,
    sent, got, passed, piece_sent, piece_got, name_sent, name_got,
):
    n_grid, n_atom = shape
    grid, atom = lax.axis_index("grid"), lax.axis_index("atom")
    meet_all(shape)
    halo = Halo(n_grid, ROUNDS, own, low, high, relay, sent, got, passed)

    def send(source, target, sent_sem, got_sem, to):
        pltpu.make_async_remote_copy(
            src_ref=source,
            dst_ref=target,
            send_sem=sent_sem,
            recv_sem=got_sem,
            device_id=to,
            device_id_type=MESH,
        ).start()

    for r in range(ROUNDS):
        halo.send(r)
    sides = ((0, 1, grid < n_grid - 1, grid > 0), (2, -1, grid > 0, grid < n_grid - 1))
    for slot, step, able, _ in sides:

        @pl.when(able)
        def _():
            send(names, all_names.at[slot], name_sent.at[slot], name_got.at[slot], (grid + step, atom))
            send(piece, beside.at[slot // 2], piece_sent.at[slot], piece_got.at[slot], (grid + step, atom))

    basis[atom] = piece[...]
    all_names[1] = names[...]

    @pl.loop(1, n_atom)
    def _(d):
        to = lax.rem(atom + d, n_atom)
        send(piece, basis.at[atom], piece_sent.at[1], piece_got.at[1], (grid, to))

    for slot, _, _, filled in sides:

        @pl.when(jnp.logical_not(filled))
        def _():
            all_names[slot] = jnp.full_like(names, -1)

    for r in range(ROUNDS):
        halo.forward(r)
    peers = pl.ds(0, n_atom - 1)
    wait_bytes(basis.at[peers], piece_got.at[1])
    wait_bytes(basis.at[peers], piece_sent.at[1])
    for slot, _, able, filled in sides:

        @pl.when(able)
        def _():
            wait_bytes(piece, piece_sent.at[slot])
            wait_bytes(names, name_sent.at[slot])

        @pl.when(filled)
        def _():
            wait_bytes(names, name_got.at[slot])
            wait_bytes(piece, piece_got.at[slot])

    halo.finish()


def halo_of(shape, own, piece, names):
    rows, columns = own.shape
    anywhere = pl.BlockSpec(memory_space=pl.ANY)
    return pl.pallas_call(
        functools.partial(halo_kernel, shape),
        out_shape=(
            jax.ShapeDtypeStruct(own.shape, own.dtype),
            jax.ShapeDtypeStruct(own.shape, own.dtype),
            jax.ShapeDtypeStruct((shape[1], *piece.shape), piece.dtype),
            jax.ShapeDtypeStruct((2, *piece.shape), piece.dtype),
            jax.ShapeDtypeStruct((3, *names.shape), names.dtype),
            jax.ShapeDtypeStruct((2, rows // 2, columns), own.dtype),
        ),
        in_specs=[anywhere, VMEM, VMEM],
        out_specs=(anywhere, anywhere, VMEM, VMEM, VMEM, anywhere),
        scratch_shapes=halo_scratch(ROUNDS)
        + [
            pltpu.SemaphoreType.DMA((3,)),
            pltpu.SemaphoreType.DMA((3,)),
            pltpu.SemaphoreType.DMA((3,)),
            pltpu.SemaphoreType.DMA((3,)),
        ],
        compiler_params=pltpu.CompilerParams(
            collective_id=1, has_side_effects=True, vmem_limit_bytes=20 << 20
        ),
        name="halo_of",
    )(own, piece, names)


def to_columns(rows):
    parts = [
        jnp.transpose(jnp.broadcast_to(rows[i : i + 1, :], (LANES, LANES)))
        for i in range(rows.shape[0])
    ]
    return jnp.concatenate(parts, axis=0)


def to_rows(columns):
    parts = []
    for i in range(columns.shape[0] // LANES):
        piece = jnp.broadcast_to(columns[i * LANES : (i + 1) * LANES, :], (LANES, LANES))
        parts.append(jnp.transpose(piece)[0:1, :])
    return jnp.concatenate(parts, axis=0)


def psi_kernel(lists, basis_t, below, own, above, psi, dens, rows, sums, basis):
    step = pl.program_id(0)
    owned = own.shape[0]
    rows[0:owned, :] = below[...]
    rows[owned : 2 * owned, :] = own[...]
    rows[2 * owned : 3 * owned, :] = above[...]
    count, points, depth = basis.shape
    picks = lists.shape[1]
    width = depth // picks
    wide = psi.shape[2]

    @pl.when(step == 0)
    def _():
        sums[...] = jnp.zeros_like(sums)
        for b in range(count):
            basis[b] = jnp.transpose(basis_t[b])

    @pl.loop(0, count)
    def _(b):
        chosen = jnp.concatenate(
            [
                rows[pl.ds(pl.multiple_of(lists[b, j] * width, width), width), :]
                for j in range(picks)
            ],
            axis=0,
        )
        value = jnp.dot(basis[b], chosen, preferred_element_type=jnp.float32)
        rounded = value.astype(jnp.bfloat16)
        psi[b] = rounded
        square = jnp.square(rounded.astype(jnp.float32))
        total = square[:, 0:LANES]
        for i in range(1, wide // LANES):
            total = total + square[:, i * LANES : (i + 1) * LANES]
        sums[b] += total

    @pl.when(step == pl.num_programs(0) - 1)
    def _():
        for b in range(count):
            dens[b : b + 1, :] = jnp.sum(jnp.transpose(sums[b]), axis=0, keepdims=True)


def psi_and_density(lists, basis_t, below, own, above):
    owned, columns = own.shape
    count, depth, points = basis_t.shape
    wide = min(columns, 512)
    grant = 2 * (9 * owned * wide + 2 * count * points * wide + 4 * count * depth * points)
    tile = pl.BlockSpec((owned, wide), lambda i, lists: (0, i))
    return pl.pallas_call(
        psi_kernel,
        out_shape=(
            jax.ShapeDtypeStruct((count, points, columns), jnp.bfloat16),
            jax.ShapeDtypeStruct((count, points), jnp.float32),
        ),
        grid_spec=pltpu.PrefetchScalarGridSpec(
            num_scalar_prefetch=1,
            grid=(columns // wide,),
            in_specs=[
                pl.BlockSpec((count, depth, points), lambda i, lists: (0, 0, 0)),
                tile,
                tile,
                tile,
            ],
            out_specs=(
                pl.BlockSpec((count, points, wide), lambda i, lists: (0, 0, i)),
                pl.BlockSpec((count, points), lambda i, lists: (0, 0)),
            ),
            scratch_shapes=[
                pltpu.VMEM((3 * owned, wide), jnp.bfloat16),
                pltpu.VMEM((count, points, LANES), jnp.float32),
                pltpu.VMEM((count, points, depth), jnp.bfloat16),
            ],
        ),
        compiler_params=pltpu.CompilerParams(vmem_limit_bytes=grant + (6 << 20)),
        cost_estimate=pl.CostEstimate(
            flops=2 * count * points * depth * columns,
            bytes_accessed=8 * owned * columns,
            transcendentals=0,
        ),
        name="psi_and_density",
    )(lists, basis_t, below, own, above)


def potential_kernel(
    shape, layers, psi, beside, dens, info, mine, hot, hot_t, weights, scale, shift, mw, aw, head,
    pot, near, psi_low, psi_high, relay, beside_t,
    dens_buf, info_buf, rows_out, rows_buf, scaled_out, scaled_buf, sent, got,
    psi_sent, psi_got, psi_passed, piece_sent, piece_got,
):
    n_grid, n_atom = shape
    n = n_grid * n_atom
    grid, atom = lax.axis_index("grid"), lax.axis_index("atom")
    me = grid * n_atom + atom

    def other(d):
        t = lax.rem(me + d, n)
        return (t // n_atom, lax.rem(t, n_atom))

    def to_all(source, held, k):
        @pl.loop(1, n)
        def _(d):
            pltpu.make_async_remote_copy(
                src_ref=source,
                dst_ref=held.at[me],
                send_sem=sent.at[k],
                recv_sem=got.at[k],
                device_id=other(d),
                device_id_type=MESH,
            ).start()

    def wait_all(held, sem, count):
        part = held.at[pl.ds(0, count)]
        pltpu.make_async_copy(part, part, sem).wait()

    meet_all(shape)
    halo = Halo(n_grid, layers + 2, psi, psi_low, psi_high, relay, psi_sent, psi_got, psi_passed)

    @pl.loop(1, n_atom)
    def _(d):
        to = lax.rem(atom + d, n_atom)
        pltpu.make_async_remote_copy(
            src_ref=dens.at[to],
            dst_ref=dens_buf.at[atom],
            send_sem=sent.at[0],
            recv_sem=got.at[0],
            device_id=(grid, to),
            device_id_type=MESH,
        ).start()

    to_all(info, info_buf, 1)
    halo.send(0)
    for slot in range(2):
        beside_t[slot, atom] = beside[slot]

        @pl.loop(1, n_atom)
        def _(d):
            to = lax.rem(atom + d, n_atom)
            pltpu.make_async_remote_copy(
                src_ref=beside.at[slot],
                dst_ref=beside_t.at[slot, atom],
                send_sem=piece_sent.at[slot],
                recv_sem=piece_got.at[slot],
                device_id=(grid, to),
                device_id_type=MESH,
            ).start()

    dens_buf[atom] = dens[atom]
    info_buf[me] = info[...]
    weight = to_columns(weights[...])[:, 0:1]

    wait_all(dens_buf, got.at[0], n_atom - 1)
    density = to_columns(2.0 * jnp.sum(dens_buf[...], axis=0))
    safe = jnp.where(density > 0.0, density, 1.0)
    radius = jnp.where(density > 0.0, jnp.exp(jnp.log(safe) * (1.0 / 3.0)), 0.0)[:, 0:1]
    hidden = jax.nn.silu(radius * scale[...] + shift[...])
    halves = hidden.shape[1] // LANES
    picks = []
    share = None
    for layer in range(layers):
        message = jax.nn.silu(
            jnp.dot(hidden.astype(jnp.bfloat16), mw[layer], preferred_element_type=jnp.float32)
        )
        weighted = (weight * message).astype(jnp.bfloat16)
        part = jnp.dot(hot_t[...], weighted, preferred_element_type=jnp.float32)
        rows_out[layer] = jnp.concatenate(
            [part[0:RUN, h * LANES : (h + 1) * LANES] for h in range(halves)], axis=0
        ).astype(jnp.bfloat16)
        to_all(rows_out.at[layer], rows_buf.at[layer], 2 + layer)
        halo.send(1 + layer)
        rows_buf[layer, me] = rows_out[layer]
        if layer == 0:
            wait_all(info_buf, got.at[1], n - 1)
            facts = info_buf[...].reshape(n * RUN, LANES)
            same = (facts[:, 0:1] == mine[...]).astype(jnp.float32)
            mass = jnp.sum(same * facts[:, LANES // 2 : LANES // 2 + 1], axis=0, keepdims=True)
            share = 1.0 / (1.0 + to_columns(mass)[:, 0:1])
            same = same.reshape(n, RUN, LANES)
            none = jnp.zeros_like(same)
            for h in range(halves):
                full = jnp.concatenate(
                    [same if k == h else none for k in range(halves)], axis=1
                ).reshape(n * RUN * halves, LANES)
                picks.append(jnp.transpose(full).astype(jnp.bfloat16))
        wait_all(rows_buf.at[layer], got.at[2 + layer], n - 1)
        halo.forward(layer)
        held = rows_buf[layer].reshape(n * RUN * halves, LANES)
        rows = jnp.concatenate(
            [jnp.dot(pick, held, preferred_element_type=jnp.float32) for pick in picks], axis=1
        )
        update = jax.nn.silu(
            jnp.dot(
                (rows * share).astype(jnp.bfloat16), aw[layer], preferred_element_type=jnp.float32
            )
        ).astype(jnp.bfloat16)
        picked = jnp.dot(hot[...], update, preferred_element_type=jnp.float32)
        hidden = hidden + message * picked
    score = jnp.sum(hidden * head[...], axis=1, keepdims=True)
    potential = radius * (1.0 + jnp.tanh(score))
    pot[...] = to_rows(potential)
    last = 2 + layers
    scaled_out[...] = to_rows(weight * potential)
    to_all(scaled_out, scaled_buf, last)
    halo.send(layers + 1)
    scaled_buf[me] = scaled_out[...]
    wait_all(scaled_buf, got.at[last], n - 1)
    halo.forward(layers)
    halo.forward(layers + 1)
    for k in range(3):
        group = jnp.clip(grid - 1 + k, 0, n_grid - 1)
        near[k * n_atom : (k + 1) * n_atom] = scaled_buf[pl.ds(group * n_atom, n_atom)]
    wait_all(dens_buf, sent.at[0], n_atom - 1)
    wait_all(info_buf, sent.at[1], n - 1)
    for layer in range(layers):
        wait_all(rows_buf.at[layer], sent.at[2 + layer], n - 1)
    wait_all(scaled_buf, sent.at[last], n - 1)
    for slot in range(2):
        wait_all(beside_t.at[slot], piece_got.at[slot], n_atom - 1)
        wait_all(beside_t.at[slot], piece_sent.at[slot], n_atom - 1)
    halo.finish()


def potential_of(shape, psi, beside, dens, info, mine, hot, hot_t, weights, scale, shift, mw, aw, head):
    n_atom, batches, points = dens.shape
    n = shape[0] * shape[1]
    layers, features, _ = mw.shape
    packed = RUN * (features // LANES)
    anywhere = pl.BlockSpec(memory_space=pl.ANY)
    return pl.pallas_call(
        functools.partial(potential_kernel, shape, layers),
        out_shape=(
            jax.ShapeDtypeStruct((batches, points), jnp.float32),
            jax.ShapeDtypeStruct((3 * n_atom, batches, points), jnp.float32),
            jax.ShapeDtypeStruct(psi.shape, psi.dtype),
            jax.ShapeDtypeStruct(psi.shape, psi.dtype),
            jax.ShapeDtypeStruct((2, psi.shape[0] // 2, *psi.shape[1:]), psi.dtype),
            jax.ShapeDtypeStruct((2, n_atom, *beside.shape[1:]), beside.dtype),
        ),
        in_specs=[anywhere] + [VMEM] * 12,
        out_specs=(VMEM, VMEM, anywhere, anywhere, anywhere, VMEM),
        scratch_shapes=[
            pltpu.VMEM((n_atom, batches, points), jnp.float32),
            pltpu.VMEM((n, RUN, LANES), jnp.float32),
            pltpu.VMEM((layers, packed, LANES), jnp.bfloat16),
            pltpu.VMEM((layers, n, packed, LANES), jnp.bfloat16),
            pltpu.VMEM((batches, points), jnp.float32),
            pltpu.VMEM((n, batches, points), jnp.float32),
            pltpu.SemaphoreType.DMA((3 + layers,)),
            pltpu.SemaphoreType.DMA((3 + layers,)),
        ]
        + halo_scratch(layers + 2)
        + [pltpu.SemaphoreType.DMA((2,)), pltpu.SemaphoreType.DMA((2,))],
        compiler_params=pltpu.CompilerParams(
            collective_id=0, has_side_effects=True, vmem_limit_bytes=30 << 20
        ),
        cost_estimate=pl.CostEstimate(
            flops=20_000_000_000, bytes_accessed=4_000_000, transcendentals=0
        ),
        name="potential_of",
    )(psi, beside, dens, info, mine, hot, hot_t, weights, scale, shift, mw, aw, head)


def fock_kernel(lists, own_t, beside_t, near, low, mid, high, out, scaled):
    step = pl.program_id(0)
    groups, count, depth, points = scaled.shape
    picks = lists.shape[1]
    width = depth // picks
    owned = out.shape[0] // width

    @pl.when(step == 0)
    def _():
        @pl.loop(0, count)
        def _(b):
            for k, values in enumerate((beside_t.at[0], own_t, beside_t.at[1])):
                scaled[k, b] = (
                    values[b].astype(jnp.float32) * near[pl.ds(k * count + b, 1), :]
                ).astype(jnp.bfloat16)

    out[...] = jnp.zeros_like(out)
    for k, psi in enumerate((low, mid, high)):

        @pl.loop(0, count)
        def _(b, k=k, psi=psi):
            for j in range(picks):
                block = lists[k * count + b, j]

                @pl.when(jnp.logical_and(block >= 0, block < owned))
                def _():
                    at = pl.ds(pl.multiple_of(block * width, width), width)
                    out[at, :] += jnp.dot(
                        scaled[k, b, j * width : (j + 1) * width, :],
                        psi[b],
                        preferred_element_type=jnp.float32,
                    )


def fock_of(lists, own_t, beside_t, near, low, mid, high, owned):
    count, depth, points = own_t.shape
    groups = 3
    columns = mid.shape[2]
    wide = min(columns, 512)
    tile = pl.BlockSpec((count, points, wide), lambda i, lists: (0, 0, i))
    grant = 2 * (9 * count * depth * points + 6 * count * points * wide + 4 * owned * wide)
    return pl.pallas_call(
        fock_kernel,
        out_shape=jax.ShapeDtypeStruct((owned, columns), jnp.float32),
        grid_spec=pltpu.PrefetchScalarGridSpec(
            num_scalar_prefetch=1,
            grid=(columns // wide,),
            in_specs=[
                pl.BlockSpec((count, depth, points), lambda i, lists: (0, 0, 0)),
                pl.BlockSpec((2, count, depth, points), lambda i, lists: (0, 0, 0, 0)),
                pl.BlockSpec((groups * count, points), lambda i, lists: (0, 0)),
                tile,
                tile,
                tile,
            ],
            out_specs=pl.BlockSpec((owned, wide), lambda i, lists: (0, i)),
            scratch_shapes=[pltpu.VMEM((groups, count, depth, points), jnp.bfloat16)],
        ),
        compiler_params=pltpu.CompilerParams(vmem_limit_bytes=grant + (4 << 20)),
        name="fock_of",
    )(lists, own_t, beside_t, near, low, mid, high)


def local(
    basis_values,
    block_lists,
    orbitals,
    point_weights,
    point_atoms,
    embed_scale,
    embed_shift,
    message_weight,
    atom_weight,
    head_weight,
):
    n_grid, n_atom = lax.axis_size("grid"), lax.axis_size("atom")
    own_rows = orbitals.shape[0]
    batches, points, depth = basis_values.shape
    width = depth // block_lists.shape[1]
    owned = own_rows // width
    shape = (n_grid, n_atom)
    first = lax.axis_index("grid") * owned
    names = jnp.pad(block_lists, ((0, 0), (0, LANES - block_lists.shape[1])))
    below, above, own_t, beside, names, _ = halo_of(
        shape, orbitals, jnp.swapaxes(basis_values, 1, 2), names
    )
    own_t = own_t.reshape(n_atom * batches, depth, points)
    lists = names[:, :, : block_lists.shape[1]].reshape(-1, block_lists.shape[1]) - first

    total = ATOM_DEV * n_atom
    lead = point_atoms[0]
    shifted = (point_atoms - lead + total // 2) % total - total // 2
    least = jnp.min(shifted)
    start = (lead + least) % total
    place = shifted - least
    lanes = jnp.arange(LANES, dtype=jnp.int32)
    onehot = place[:, None] == lanes[None, :]
    hot = onehot.astype(jnp.bfloat16)
    hot_t = (place[None, :] == lanes[:, None]).astype(jnp.bfloat16)
    mass = jnp.sum(jnp.where(onehot, point_weights[:, None], 0.0), axis=0)[:RUN]
    names = ((start + lanes) % total).astype(jnp.float32)
    mine = jnp.where(lanes < RUN, names, -1.0)[None, :]
    info = jnp.where(lanes[None, :] < LANES // 2, names[:RUN, None], mass[:, None])

    psi, dens = psi_and_density(block_lists - first + owned, own_t, below, orbitals, above)
    potential, near, psi_low, psi_high, _, beside_t = potential_of(
        shape,
        psi,
        beside,
        dens.reshape(n_atom, batches, points),
        info,
        mine,
        hot,
        hot_t,
        point_weights.reshape(batches, points),
        embed_scale[None, :],
        embed_shift[None, :],
        message_weight,
        atom_weight,
        head_weight[None, :],
    )
    fock = fock_of(
        lists, own_t, beside_t.reshape(2, *own_t.shape), near.reshape(-1, points),
        psi_low, psi, psi_high, own_rows,
    )
    return (fock, potential.reshape(-1))


def solution(mesh):
    return jax.shard_map(
        local,
        mesh=mesh,
        in_specs=(
            P(("grid", "atom"), None, None),
            P("grid", None),
            P("grid", "atom"),
            P(("grid", "atom")),
            P(("grid", "atom")),
            P(),
            P(),
            P(),
            P(),
            P(),
        ),
        out_specs=(P("grid", "atom"), P(("grid", "atom"))),
        check_vma=False,
    )
```

```python
import functools
import jax
import jax.numpy as jnp
from jax import lax
from jax.experimental import pallas as pl
from jax.experimental.pallas import tpu as pltpu
from jax.sharding import PartitionSpec as P

ATOM_DEV = 32
RUN = max(ATOM_DEV // 4, 1)
LANES = 128
VMEM = pl.BlockSpec(memory_space=pltpu.VMEM)
MESH = pl.DeviceIdType.MESH


def wait_bytes(ref, sem):
    pltpu.make_async_copy(ref, ref, sem).wait()


class Halo:
    def __init__(self, n_grid, rounds, source, low, high, relay, sent, got, passed):
        self.n_grid, self.rounds, self.middle = n_grid, rounds, n_grid // 2
        self.source, self.low, self.high, self.relay = source, low, high, relay
        self.sent, self.got, self.passed = sent, got, passed
        self.size = source.shape[0] // (2 * rounds)
        self.grid, self.atom = lax.axis_index("grid"), lax.axis_index("atom")

    def copy(self, source, target, sent, got, grid):
        pltpu.make_async_remote_copy(
            src_ref=source,
            dst_ref=target,
            send_sem=sent,
            recv_sem=got,
            device_id=(grid, self.atom),
            device_id_type=MESH,
        ).start()

    def send(self, r):
        grid, last, size = self.grid, self.n_grid - 1, self.size
        for way, (step, held, split, able) in enumerate(
            (
                (1, self.low, self.middle - 1, grid < last),
                (-1, self.high, self.middle, grid > 0),
            )
        ):
            for side, end in enumerate((0, last)):
                part = pl.ds((side * self.rounds + r) * size, size)

                @pl.when(jnp.logical_and(able, grid != split))
                def _():
                    self.copy(
                        self.source.at[part], held.at[part],
                        self.sent.at[way], self.got.at[way], grid + step,
                    )

                @pl.when(grid == split)
                def _():
                    self.copy(
                        self.source.at[part], self.relay.at[way, pl.ds(r * size, size)],
                        self.sent.at[way], self.passed.at[way, r], end,
                    )

    def forward(self, r):
        size = self.size
        for side, end in enumerate((0, self.n_grid - 1)):

            @pl.when(self.grid == end)
            def _():
                for way, (held, to) in enumerate(
                    ((self.low, self.middle), (self.high, self.middle - 1))
                ):
                    piece = self.relay.at[way, pl.ds(r * size, size)]
                    wait_bytes(piece, self.passed.at[way, r])
                    part = pl.ds((side * self.rounds + r) * size, size)
                    self.copy(piece, held.at[part], self.sent.at[2 + way], self.got.at[way], to)

    def finish(self):
        grid, last = self.grid, self.n_grid - 1

        @pl.when(grid > 0)
        def _():
            wait_bytes(self.low, self.got.at[0])
            wait_bytes(self.source, self.sent.at[1])

        @pl.when(grid < last)
        def _():
            wait_bytes(self.high, self.got.at[1])
            wait_bytes(self.source, self.sent.at[0])

        @pl.when(jnp.logical_or(grid == 0, grid == last))
        def _():
            for way in range(2):
                wait_bytes(self.relay.at[way], self.sent.at[2 + way])


def halo_scratch(rounds):
    return [
        pltpu.SemaphoreType.DMA((4,)),
        pltpu.SemaphoreType.DMA((2,)),
        pltpu.SemaphoreType.DMA((2, rounds)),
    ]


def meet_all(shape):
    n_grid, n_atom = shape
    n = n_grid * n_atom
    me = lax.axis_index("grid") * n_atom + lax.axis_index("atom")
    barrier = pltpu.get_barrier_semaphore()

    @pl.loop(1, n)
    def _(d):
        t = lax.rem(me + d, n)
        pl.semaphore_signal(
            barrier, inc=1, device_id=(t // n_atom, lax.rem(t, n_atom)), device_id_type=MESH
        )

    pl.semaphore_wait(barrier, n - 1)


ROUNDS = 4


def halo_kernel(
    shape, own, piece, names, low, high, basis, all_names, relay,
    sent, got, passed, piece_sent, piece_got, name_sent, name_got, line_sent, line_got,
):
    n_grid, n_atom = shape
    grid, atom = lax.axis_index("grid"), lax.axis_index("atom")
    meet_all(shape)
    halo = Halo(n_grid, ROUNDS, own, low, high, relay, sent, got, passed)

    def send(source, target, sent_sem, got_sem, to):
        pltpu.make_async_remote_copy(
            src_ref=source,
            dst_ref=target,
            send_sem=sent_sem,
            recv_sem=got_sem,
            device_id=to,
            device_id_type=MESH,
        ).start()

    sides = ((0, 1, grid < n_grid - 1, grid > 0), (2, -1, grid > 0, grid < n_grid - 1))
    for slot, step, able, _ in sides:

        @pl.when(able)
        def _():
            send(names, all_names.at[slot], name_sent.at[slot], name_got.at[slot], (grid + step, atom))
            send(piece, basis.at[slot, atom], piece_sent.at[slot], piece_got.at[slot], (grid + step, atom))

    for r in range(ROUNDS):
        halo.send(r)

    def line(slot, d, way):
        origin = atom - (d - 1) if way == 0 else atom + (d - 1)
        able = (
            jnp.logical_and(atom < n_atom - 1, atom >= d - 1)
            if way == 0
            else jnp.logical_and(atom > 0, atom + d - 1 < n_atom)
        )
        return jnp.clip(origin, 0, n_atom - 1), able

    filled_of = {0: grid > 0, 1: grid >= 0, 2: grid < n_grid - 1}

    def line_send(slot, d):
        for way in range(2):
            origin, able = line(slot, d, way)

            @pl.when(jnp.logical_and(able, filled_of[slot]))
            def _():
                source = piece if slot == 1 and d == 1 else basis.at[slot, origin]
                send(
                    source, basis.at[slot, origin], line_sent.at[slot, way, d - 1],
                    line_got.at[slot, way, d - 1], (grid, atom + 1 - 2 * way),
                )

    def line_wait(slot, d, sems, arrived):
        for way in range(2):
            if arrived:
                able = atom >= d if way == 0 else atom + d < n_atom
            else:
                able = line(slot, d, way)[1]

            @pl.when(jnp.logical_and(able, filled_of[slot]))
            def _():
                wait_bytes(piece, sems.at[slot, way, d - 1])

    line_send(1, 1)
    basis[1, atom] = piece[...]
    all_names[1] = names[...]
    for slot, _, _, filled in sides:

        @pl.when(filled)
        def _():
            wait_bytes(piece, piece_got.at[slot])

        @pl.when(jnp.logical_not(filled))
        def _():
            all_names[slot] = jnp.full_like(names, -1)

    line_send(0, 1)
    line_send(2, 1)
    moved = 0
    for d in range(1, n_atom):
        for slot in (1, 0, 2):
            line_wait(slot, d, line_got, True)
            if d < n_atom - 1:
                line_send(slot, d + 1)
        while moved < ROUNDS and moved < (d * ROUNDS) // (n_atom - 1):
            halo.forward(moved)
            moved += 1
    for d in range(1, n_atom):
        for slot in (1, 0, 2):
            line_wait(slot, d, line_sent, False)
    for slot, _, able, filled in sides:

        @pl.when(able)
        def _():
            wait_bytes(piece, piece_sent.at[slot])
            wait_bytes(names, name_sent.at[slot])

        @pl.when(filled)
        def _():
            wait_bytes(names, name_got.at[slot])

    halo.finish()


def halo_of(shape, own, piece, names):
    rows, columns = own.shape
    anywhere = pl.BlockSpec(memory_space=pl.ANY)
    return pl.pallas_call(
        functools.partial(halo_kernel, shape),
        out_shape=(
            jax.ShapeDtypeStruct(own.shape, own.dtype),
            jax.ShapeDtypeStruct(own.shape, own.dtype),
            jax.ShapeDtypeStruct((3, shape[1], *piece.shape), piece.dtype),
            jax.ShapeDtypeStruct((3, *names.shape), names.dtype),
            jax.ShapeDtypeStruct((2, rows // 2, columns), own.dtype),
        ),
        in_specs=[anywhere, VMEM, VMEM],
        out_specs=(anywhere, anywhere, VMEM, VMEM, anywhere),
        scratch_shapes=halo_scratch(ROUNDS)
        + [
            pltpu.SemaphoreType.DMA((3,)),
            pltpu.SemaphoreType.DMA((3,)),
            pltpu.SemaphoreType.DMA((3,)),
            pltpu.SemaphoreType.DMA((3,)),
            pltpu.SemaphoreType.DMA((3, 2, shape[1] - 1)),
            pltpu.SemaphoreType.DMA((3, 2, shape[1] - 1)),
        ],
        compiler_params=pltpu.CompilerParams(
            collective_id=1, has_side_effects=True, vmem_limit_bytes=24 << 20
        ),
        name="halo_of",
    )(own, piece, names)


def to_columns(rows):
    parts = [
        jnp.transpose(jnp.broadcast_to(rows[i : i + 1, :], (LANES, LANES)))
        for i in range(rows.shape[0])
    ]
    return jnp.concatenate(parts, axis=0)


def to_rows(columns):
    parts = []
    for i in range(columns.shape[0] // LANES):
        piece = jnp.broadcast_to(columns[i * LANES : (i + 1) * LANES, :], (LANES, LANES))
        parts.append(jnp.transpose(piece)[0:1, :])
    return jnp.concatenate(parts, axis=0)


def psi_kernel(lists, basis_t, below, own, above, psi, dens, rows, sums, basis):
    step = pl.program_id(0)
    owned = own.shape[0]
    rows[0:owned, :] = below[...]
    rows[owned : 2 * owned, :] = own[...]
    rows[2 * owned : 3 * owned, :] = above[...]
    count, points, depth = basis.shape
    picks = lists.shape[1]
    width = depth // picks
    wide = psi.shape[2]

    @pl.when(step == 0)
    def _():
        sums[...] = jnp.zeros_like(sums)
        for b in range(count):
            basis[b] = jnp.transpose(basis_t[0, b])

    @pl.loop(0, count)
    def _(b):
        chosen = jnp.concatenate(
            [
                rows[pl.ds(pl.multiple_of(lists[b, j] * width, width), width), :]
                for j in range(picks)
            ],
            axis=0,
        )
        value = jnp.dot(basis[b], chosen, preferred_element_type=jnp.float32)
        rounded = value.astype(jnp.bfloat16)
        psi[b] = rounded
        square = jnp.square(rounded.astype(jnp.float32))
        total = square[:, 0:LANES]
        for i in range(1, wide // LANES):
            total = total + square[:, i * LANES : (i + 1) * LANES]
        sums[b] += total

    @pl.when(step == pl.num_programs(0) - 1)
    def _():
        for b in range(count):
            dens[b : b + 1, :] = jnp.sum(jnp.transpose(sums[b]), axis=0, keepdims=True)


def psi_and_density(lists, basis_t, below, own, above):
    owned, columns = own.shape
    _, count, depth, points = basis_t.shape
    wide = min(columns, 512)
    grant = 2 * (9 * owned * wide + 2 * count * points * wide + 4 * count * depth * points)
    tile = pl.BlockSpec((owned, wide), lambda i, lists: (0, i))
    return pl.pallas_call(
        psi_kernel,
        out_shape=(
            jax.ShapeDtypeStruct((count, points, columns), jnp.bfloat16),
            jax.ShapeDtypeStruct((count, points), jnp.float32),
        ),
        grid_spec=pltpu.PrefetchScalarGridSpec(
            num_scalar_prefetch=1,
            grid=(columns // wide,),
            in_specs=[
                pl.BlockSpec((1, count, depth, points), lambda i, lists: (1, 0, 0, 0)),
                tile,
                tile,
                tile,
            ],
            out_specs=(
                pl.BlockSpec((count, points, wide), lambda i, lists: (0, 0, i)),
                pl.BlockSpec((count, points), lambda i, lists: (0, 0)),
            ),
            scratch_shapes=[
                pltpu.VMEM((3 * owned, wide), jnp.bfloat16),
                pltpu.VMEM((count, points, LANES), jnp.float32),
                pltpu.VMEM((count, points, depth), jnp.bfloat16),
            ],
        ),
        compiler_params=pltpu.CompilerParams(vmem_limit_bytes=grant + (6 << 20)),
        cost_estimate=pl.CostEstimate(
            flops=2 * count * points * depth * columns,
            bytes_accessed=8 * owned * columns,
            transcendentals=0,
        ),
        name="psi_and_density",
    )(lists, basis_t, below, own, above)


def potential_kernel(
    shape, layers, psi, dens, info, mine, hot, hot_t, weights, scale, shift, mw, aw, head,
    pot, near, psi_low, psi_high, relay,
    dens_buf, info_buf, rows_out, rows_buf, scaled_out, scaled_buf, sent, got,
    psi_sent, psi_got, psi_passed,
):
    n_grid, n_atom = shape
    n = n_grid * n_atom
    grid, atom = lax.axis_index("grid"), lax.axis_index("atom")
    me = grid * n_atom + atom

    def other(d):
        t = lax.rem(me + d, n)
        return (t // n_atom, lax.rem(t, n_atom))

    def to_all(source, held, k):
        @pl.loop(1, n)
        def _(d):
            pltpu.make_async_remote_copy(
                src_ref=source,
                dst_ref=held.at[me],
                send_sem=sent.at[k],
                recv_sem=got.at[k],
                device_id=other(d),
                device_id_type=MESH,
            ).start()

    def wait_all(held, sem, count):
        part = held.at[pl.ds(0, count)]
        pltpu.make_async_copy(part, part, sem).wait()

    meet_all(shape)
    halo = Halo(n_grid, layers + 2, psi, psi_low, psi_high, relay, psi_sent, psi_got, psi_passed)

    @pl.loop(1, n_atom)
    def _(d):
        to = lax.rem(atom + d, n_atom)
        pltpu.make_async_remote_copy(
            src_ref=dens.at[to],
            dst_ref=dens_buf.at[atom],
            send_sem=sent.at[0],
            recv_sem=got.at[0],
            device_id=(grid, to),
            device_id_type=MESH,
        ).start()

    to_all(info, info_buf, 1)
    halo.send(0)
    dens_buf[atom] = dens[atom]
    info_buf[me] = info[...]
    weight = to_columns(weights[...])[:, 0:1]

    wait_all(dens_buf, got.at[0], n_atom - 1)
    density = to_columns(2.0 * jnp.sum(dens_buf[...], axis=0))
    safe = jnp.where(density > 0.0, density, 1.0)
    radius = jnp.where(density > 0.0, jnp.exp(jnp.log(safe) * (1.0 / 3.0)), 0.0)[:, 0:1]
    hidden = jax.nn.silu(radius * scale[...] + shift[...])
    halves = hidden.shape[1] // LANES
    picks = []
    share = None
    for layer in range(layers):
        message = jax.nn.silu(
            jnp.dot(hidden.astype(jnp.bfloat16), mw[layer], preferred_element_type=jnp.float32)
        )
        weighted = (weight * message).astype(jnp.bfloat16)
        part = jnp.dot(hot_t[...], weighted, preferred_element_type=jnp.float32)
        rows_out[layer] = jnp.concatenate(
            [part[0:RUN, h * LANES : (h + 1) * LANES] for h in range(halves)], axis=0
        ).astype(jnp.bfloat16)
        to_all(rows_out.at[layer], rows_buf.at[layer], 2 + layer)
        halo.send(1 + layer)
        rows_buf[layer, me] = rows_out[layer]
        if layer == 0:
            wait_all(info_buf, got.at[1], n - 1)
            facts = info_buf[...].reshape(n * RUN, LANES)
            same = (facts[:, 0:1] == mine[...]).astype(jnp.float32)
            mass = jnp.sum(same * facts[:, LANES // 2 : LANES // 2 + 1], axis=0, keepdims=True)
            share = 1.0 / (1.0 + to_columns(mass)[:, 0:1])
            same = same.reshape(n, RUN, LANES)
            none = jnp.zeros_like(same)
            for h in range(halves):
                full = jnp.concatenate(
                    [same if k == h else none for k in range(halves)], axis=1
                ).reshape(n * RUN * halves, LANES)
                picks.append(jnp.transpose(full).astype(jnp.bfloat16))
        wait_all(rows_buf.at[layer], got.at[2 + layer], n - 1)
        halo.forward(layer)
        held = rows_buf[layer].reshape(n * RUN * halves, LANES)
        rows = jnp.concatenate(
            [jnp.dot(pick, held, preferred_element_type=jnp.float32) for pick in picks], axis=1
        )
        update = jax.nn.silu(
            jnp.dot(
                (rows * share).astype(jnp.bfloat16), aw[layer], preferred_element_type=jnp.float32
            )
        ).astype(jnp.bfloat16)
        picked = jnp.dot(hot[...], update, preferred_element_type=jnp.float32)
        hidden = hidden + message * picked
    score = jnp.sum(hidden * head[...], axis=1, keepdims=True)
    potential = radius * (1.0 + jnp.tanh(score))
    pot[...] = to_rows(potential)
    last = 2 + layers
    scaled_out[...] = to_rows(weight * potential)
    to_all(scaled_out, scaled_buf, last)
    halo.send(layers + 1)
    scaled_buf[me] = scaled_out[...]
    wait_all(scaled_buf, got.at[last], n - 1)
    halo.forward(layers)
    halo.forward(layers + 1)
    for k in range(3):
        group = jnp.clip(grid - 1 + k, 0, n_grid - 1)
        near[k * n_atom : (k + 1) * n_atom] = scaled_buf[pl.ds(group * n_atom, n_atom)]
    wait_all(dens_buf, sent.at[0], n_atom - 1)
    wait_all(info_buf, sent.at[1], n - 1)
    for layer in range(layers):
        wait_all(rows_buf.at[layer], sent.at[2 + layer], n - 1)
    wait_all(scaled_buf, sent.at[last], n - 1)
    halo.finish()


def potential_of(shape, psi, dens, info, mine, hot, hot_t, weights, scale, shift, mw, aw, head):
    n_atom, batches, points = dens.shape
    n = shape[0] * shape[1]
    layers, features, _ = mw.shape
    packed = RUN * (features // LANES)
    anywhere = pl.BlockSpec(memory_space=pl.ANY)
    return pl.pallas_call(
        functools.partial(potential_kernel, shape, layers),
        out_shape=(
            jax.ShapeDtypeStruct((batches, points), jnp.float32),
            jax.ShapeDtypeStruct((3 * n_atom, batches, points), jnp.float32),
            jax.ShapeDtypeStruct(psi.shape, psi.dtype),
            jax.ShapeDtypeStruct(psi.shape, psi.dtype),
            jax.ShapeDtypeStruct((2, psi.shape[0] // 2, *psi.shape[1:]), psi.dtype),
        ),
        in_specs=[anywhere] + [VMEM] * 11,
        out_specs=(VMEM, VMEM, anywhere, anywhere, anywhere),
        scratch_shapes=[
            pltpu.VMEM((n_atom, batches, points), jnp.float32),
            pltpu.VMEM((n, RUN, LANES), jnp.float32),
            pltpu.VMEM((layers, packed, LANES), jnp.bfloat16),
            pltpu.VMEM((layers, n, packed, LANES), jnp.bfloat16),
            pltpu.VMEM((batches, points), jnp.float32),
            pltpu.VMEM((n, batches, points), jnp.float32),
            pltpu.SemaphoreType.DMA((3 + layers,)),
            pltpu.SemaphoreType.DMA((3 + layers,)),
        ]
        + halo_scratch(layers + 2),
        compiler_params=pltpu.CompilerParams(
            collective_id=0, has_side_effects=True, vmem_limit_bytes=24 << 20
        ),
        cost_estimate=pl.CostEstimate(
            flops=20_000_000_000, bytes_accessed=4_000_000, transcendentals=0
        ),
        name="potential_of",
    )(psi, dens, info, mine, hot, hot_t, weights, scale, shift, mw, aw, head)


def fock_kernel(lists, basis_t, near, low, mid, high, out, scaled):
    step = pl.program_id(0)
    groups, count, depth, points = basis_t.shape
    picks = lists.shape[1]
    width = depth // picks
    owned = out.shape[0] // width

    @pl.when(step == 0)
    def _():
        @pl.loop(0, groups)
        def _(k):
            @pl.loop(0, count)
            def _(b):
                scaled[k, b] = (
                    basis_t[k, b].astype(jnp.float32) * near[pl.ds(k * count + b, 1), :]
                ).astype(jnp.bfloat16)

    out[...] = jnp.zeros_like(out)
    for k, psi in enumerate((low, mid, high)):

        @pl.loop(0, count)
        def _(b, k=k, psi=psi):
            for j in range(picks):
                block = lists[k * count + b, j]

                @pl.when(jnp.logical_and(block >= 0, block < owned))
                def _():
                    at = pl.ds(pl.multiple_of(block * width, width), width)
                    out[at, :] += jnp.dot(
                        scaled[k, b, j * width : (j + 1) * width, :],
                        psi[b],
                        preferred_element_type=jnp.float32,
                    )


def fock_of(lists, basis_t, near, low, mid, high, owned):
    groups, count, depth, points = basis_t.shape
    columns = mid.shape[2]
    wide = min(columns, 512)
    tile = pl.BlockSpec((count, points, wide), lambda i, lists: (0, 0, i))
    grant = 2 * (9 * count * depth * points + 6 * count * points * wide + 4 * owned * wide)
    return pl.pallas_call(
        fock_kernel,
        out_shape=jax.ShapeDtypeStruct((owned, columns), jnp.float32),
        grid_spec=pltpu.PrefetchScalarGridSpec(
            num_scalar_prefetch=1,
            grid=(columns // wide,),
            in_specs=[
                pl.BlockSpec((groups, count, depth, points), lambda i, lists: (0, 0, 0, 0)),
                pl.BlockSpec((groups * count, points), lambda i, lists: (0, 0)),
                tile,
                tile,
                tile,
            ],
            out_specs=pl.BlockSpec((owned, wide), lambda i, lists: (0, i)),
            scratch_shapes=[pltpu.VMEM((groups, count, depth, points), jnp.bfloat16)],
        ),
        compiler_params=pltpu.CompilerParams(vmem_limit_bytes=grant + (4 << 20)),
        name="fock_of",
    )(lists, basis_t, near, low, mid, high)


def local(
    basis_values,
    block_lists,
    orbitals,
    point_weights,
    point_atoms,
    embed_scale,
    embed_shift,
    message_weight,
    atom_weight,
    head_weight,
):
    n_grid, n_atom = lax.axis_size("grid"), lax.axis_size("atom")
    own_rows = orbitals.shape[0]
    batches, points, depth = basis_values.shape
    width = depth // block_lists.shape[1]
    owned = own_rows // width
    shape = (n_grid, n_atom)
    first = lax.axis_index("grid") * owned
    names = jnp.pad(block_lists, ((0, 0), (0, LANES - block_lists.shape[1])))
    below, above, basis_t, names, _ = halo_of(
        shape, orbitals, jnp.swapaxes(basis_values, 1, 2), names
    )
    basis_t = basis_t.reshape(3, n_atom * batches, depth, points)
    lists = names[:, :, : block_lists.shape[1]].reshape(-1, block_lists.shape[1]) - first

    total = ATOM_DEV * n_atom
    lead = point_atoms[0]
    shifted = (point_atoms - lead + total // 2) % total - total // 2
    least = jnp.min(shifted)
    start = (lead + least) % total
    place = shifted - least
    lanes = jnp.arange(LANES, dtype=jnp.int32)
    onehot = place[:, None] == lanes[None, :]
    hot = onehot.astype(jnp.bfloat16)
    hot_t = (place[None, :] == lanes[:, None]).astype(jnp.bfloat16)
    mass = jnp.sum(jnp.where(onehot, point_weights[:, None], 0.0), axis=0)[:RUN]
    names = ((start + lanes) % total).astype(jnp.float32)
    mine = jnp.where(lanes < RUN, names, -1.0)[None, :]
    info = jnp.where(lanes[None, :] < LANES // 2, names[:RUN, None], mass[:, None])

    psi, dens = psi_and_density(block_lists - first + owned, basis_t, below, orbitals, above)
    potential, near, psi_low, psi_high, _ = potential_of(
        shape,
        psi,
        dens.reshape(n_atom, batches, points),
        info,
        mine,
        hot,
        hot_t,
        point_weights.reshape(batches, points),
        embed_scale[None, :],
        embed_shift[None, :],
        message_weight,
        atom_weight,
        head_weight[None, :],
    )
    fock = fock_of(
        lists, basis_t, near.reshape(-1, points), psi_low, psi, psi_high, own_rows
    )
    return (fock, potential.reshape(-1))


def solution(mesh):
    return jax.shard_map(
        local,
        mesh=mesh,
        in_specs=(
            P(("grid", "atom"), None, None),
            P("grid", None),
            P("grid", "atom"),
            P(("grid", "atom")),
            P(("grid", "atom")),
            P(),
            P(),
            P(),
            P(),
            P(),
        ),
        out_specs=(P("grid", "atom"), P(("grid", "atom"))),
        check_vma=False,
    )
```

```python
import functools
import jax
import jax.numpy as jnp
from jax import lax
from jax.experimental import pallas as pl
from jax.experimental.pallas import tpu as pltpu
from jax.sharding import PartitionSpec as P

ATOM_DEV = 32
RUN = max(ATOM_DEV // 4, 1)
LANES = 128
VMEM = pl.BlockSpec(memory_space=pltpu.VMEM)
MESH = pl.DeviceIdType.MESH


def wait_bytes(ref, sem):
    pltpu.make_async_copy(ref, ref, sem).wait()


class Halo:
    def __init__(self, n_grid, rounds, source, low, high, relay, sent, got, passed):
        self.n_grid, self.rounds, self.middle = n_grid, rounds, n_grid // 2
        self.source, self.low, self.high, self.relay = source, low, high, relay
        self.sent, self.got, self.passed = sent, got, passed
        self.size = source.shape[0] // (2 * rounds)
        self.grid, self.atom = lax.axis_index("grid"), lax.axis_index("atom")

    def copy(self, source, target, sent, got, grid):
        pltpu.make_async_remote_copy(
            src_ref=source,
            dst_ref=target,
            send_sem=sent,
            recv_sem=got,
            device_id=(grid, self.atom),
            device_id_type=MESH,
        ).start()

    def send(self, r):
        grid, last, size = self.grid, self.n_grid - 1, self.size
        for way, (step, held, split, able) in enumerate(
            (
                (1, self.low, self.middle - 1, grid < last),
                (-1, self.high, self.middle, grid > 0),
            )
        ):
            for side, end in enumerate((0, last)):
                part = pl.ds((side * self.rounds + r) * size, size)

                @pl.when(jnp.logical_and(able, grid != split))
                def _():
                    self.copy(
                        self.source.at[part], held.at[part],
                        self.sent.at[way], self.got.at[way], grid + step,
                    )

                @pl.when(grid == split)
                def _():
                    self.copy(
                        self.source.at[part], self.relay.at[way, pl.ds(r * size, size)],
                        self.sent.at[way], self.passed.at[way, r], end,
                    )

    def forward(self, r):
        size = self.size
        for side, end in enumerate((0, self.n_grid - 1)):

            @pl.when(self.grid == end)
            def _():
                for way, (held, to) in enumerate(
                    ((self.low, self.middle), (self.high, self.middle - 1))
                ):
                    piece = self.relay.at[way, pl.ds(r * size, size)]
                    wait_bytes(piece, self.passed.at[way, r])
                    part = pl.ds((side * self.rounds + r) * size, size)
                    self.copy(piece, held.at[part], self.sent.at[2 + way], self.got.at[way], to)

    def finish(self):
        grid, last = self.grid, self.n_grid - 1

        @pl.when(grid > 0)
        def _():
            wait_bytes(self.low, self.got.at[0])
            wait_bytes(self.source, self.sent.at[1])

        @pl.when(grid < last)
        def _():
            wait_bytes(self.high, self.got.at[1])
            wait_bytes(self.source, self.sent.at[0])

        @pl.when(jnp.logical_or(grid == 0, grid == last))
        def _():
            for way in range(2):
                wait_bytes(self.relay.at[way], self.sent.at[2 + way])


def halo_scratch(rounds):
    return [
        pltpu.SemaphoreType.DMA((4,)),
        pltpu.SemaphoreType.DMA((2,)),
        pltpu.SemaphoreType.DMA((2, rounds)),
    ]


def meet_all(shape):
    n_grid, n_atom = shape
    n = n_grid * n_atom
    me = lax.axis_index("grid") * n_atom + lax.axis_index("atom")
    barrier = pltpu.get_barrier_semaphore()

    @pl.loop(1, n)
    def _(d):
        t = lax.rem(me + d, n)
        pl.semaphore_signal(
            barrier, inc=1, device_id=(t // n_atom, lax.rem(t, n_atom)), device_id_type=MESH
        )

    pl.semaphore_wait(barrier, n - 1)


ROUNDS = 4


def halo_kernel(
    shape, own, piece, names, low, high, basis, all_names, relay,
    sent, got, passed, piece_sent, piece_got, name_sent, name_got, line_sent, line_got,
):
    n_grid, n_atom = shape
    grid, atom = lax.axis_index("grid"), lax.axis_index("atom")
    meet_all(shape)
    halo = Halo(n_grid, ROUNDS, own, low, high, relay, sent, got, passed)

    def send(source, target, sent_sem, got_sem, to):
        pltpu.make_async_remote_copy(
            src_ref=source,
            dst_ref=target,
            send_sem=sent_sem,
            recv_sem=got_sem,
            device_id=to,
            device_id_type=MESH,
        ).start()

    sides = ((0, 1, grid < n_grid - 1, grid > 0), (2, -1, grid > 0, grid < n_grid - 1))
    for slot, step, able, _ in sides:

        @pl.when(able)
        def _():
            send(names, all_names.at[slot], name_sent.at[slot], name_got.at[slot], (grid + step, atom))
            send(piece, basis.at[slot, atom], piece_sent.at[slot], piece_got.at[slot], (grid + step, atom))

    for r in range(ROUNDS):
        halo.send(r)

    def line(slot, d, way):
        origin = atom - (d - 1) if way == 0 else atom + (d - 1)
        able = (
            jnp.logical_and(atom < n_atom - 1, atom >= d - 1)
            if way == 0
            else jnp.logical_and(atom > 0, atom + d - 1 < n_atom)
        )
        return jnp.clip(origin, 0, n_atom - 1), able

    filled_of = {0: grid > 0, 1: grid >= 0, 2: grid < n_grid - 1}

    def line_send(slot, d):
        for way in range(2):
            origin, able = line(slot, d, way)

            @pl.when(jnp.logical_and(able, filled_of[slot]))
            def _():
                source = piece if slot == 1 and d == 1 else basis.at[slot, origin]
                send(
                    source, basis.at[slot, origin], line_sent.at[slot, way, d - 1],
                    line_got.at[slot, way, d - 1], (grid, atom + 1 - 2 * way),
                )

    def line_wait(slot, d, sems, arrived):
        for way in range(2):
            if arrived:
                able = atom >= d if way == 0 else atom + d < n_atom
            else:
                able = line(slot, d, way)[1]

            @pl.when(jnp.logical_and(able, filled_of[slot]))
            def _():
                wait_bytes(piece, sems.at[slot, way, d - 1])

    line_send(1, 1)
    basis[1, atom] = piece[...]
    all_names[1] = names[...]
    for slot, _, _, filled in sides:

        @pl.when(filled)
        def _():
            wait_bytes(piece, piece_got.at[slot])

        @pl.when(jnp.logical_not(filled))
        def _():
            all_names[slot] = jnp.full_like(names, -1)

    line_send(0, 1)
    line_send(2, 1)
    moved = 0
    for d in range(1, n_atom):
        for slot in (1, 0, 2):
            line_wait(slot, d, line_got, True)
            if d < n_atom - 1:
                line_send(slot, d + 1)
        while moved < ROUNDS and moved < (d * ROUNDS) // (n_atom - 1):
            halo.forward(moved)
            moved += 1
    for d in range(1, n_atom):
        for slot in (1, 0, 2):
            line_wait(slot, d, line_sent, False)
    for slot, _, able, filled in sides:

        @pl.when(able)
        def _():
            wait_bytes(piece, piece_sent.at[slot])
            wait_bytes(names, name_sent.at[slot])

        @pl.when(filled)
        def _():
            wait_bytes(names, name_got.at[slot])

    halo.finish()


def halo_of(shape, own, piece, names):
    rows, columns = own.shape
    anywhere = pl.BlockSpec(memory_space=pl.ANY)
    return pl.pallas_call(
        functools.partial(halo_kernel, shape),
        out_shape=(
            jax.ShapeDtypeStruct(own.shape, own.dtype),
            jax.ShapeDtypeStruct(own.shape, own.dtype),
            jax.ShapeDtypeStruct((3, shape[1], *piece.shape), piece.dtype),
            jax.ShapeDtypeStruct((3, *names.shape), names.dtype),
            jax.ShapeDtypeStruct((2, rows // 2, columns), own.dtype),
        ),
        in_specs=[anywhere, VMEM, VMEM],
        out_specs=(anywhere, anywhere, VMEM, VMEM, anywhere),
        scratch_shapes=halo_scratch(ROUNDS)
        + [
            pltpu.SemaphoreType.DMA((3,)),
            pltpu.SemaphoreType.DMA((3,)),
            pltpu.SemaphoreType.DMA((3,)),
            pltpu.SemaphoreType.DMA((3,)),
            pltpu.SemaphoreType.DMA((3, 2, shape[1] - 1)),
            pltpu.SemaphoreType.DMA((3, 2, shape[1] - 1)),
        ],
        compiler_params=pltpu.CompilerParams(
            collective_id=1, has_side_effects=True, vmem_limit_bytes=24 << 20
        ),
        name="halo_of",
    )(own, piece, names)


def to_columns(rows):
    parts = [
        jnp.transpose(jnp.broadcast_to(rows[i : i + 1, :], (LANES, LANES)))
        for i in range(rows.shape[0])
    ]
    return jnp.concatenate(parts, axis=0)


def to_rows(columns):
    parts = []
    for i in range(columns.shape[0] // LANES):
        piece = jnp.broadcast_to(columns[i * LANES : (i + 1) * LANES, :], (LANES, LANES))
        parts.append(jnp.transpose(piece)[0:1, :])
    return jnp.concatenate(parts, axis=0)


def psi_kernel(lists, basis_t, below, own, above, psi, dens, rows, sums, basis):
    step = pl.program_id(0)
    owned = own.shape[0]
    rows[0:owned, :] = below[...]
    rows[owned : 2 * owned, :] = own[...]
    rows[2 * owned : 3 * owned, :] = above[...]
    count, points, depth = basis.shape
    picks = lists.shape[1]
    width = depth // picks
    wide = psi.shape[2]

    @pl.when(step == 0)
    def _():
        sums[...] = jnp.zeros_like(sums)
        for b in range(count):
            basis[b] = jnp.transpose(basis_t[0, b])

    @pl.loop(0, count)
    def _(b):
        chosen = jnp.concatenate(
            [
                rows[pl.ds(pl.multiple_of(lists[b, j] * width, width), width), :]
                for j in range(picks)
            ],
            axis=0,
        )
        value = jnp.dot(basis[b], chosen, preferred_element_type=jnp.float32)
        rounded = value.astype(jnp.bfloat16)
        psi[b] = rounded
        square = jnp.square(rounded.astype(jnp.float32))
        total = square[:, 0:LANES]
        for i in range(1, wide // LANES):
            total = total + square[:, i * LANES : (i + 1) * LANES]
        sums[b] += total

    @pl.when(step == pl.num_programs(0) - 1)
    def _():
        for b in range(count):
            dens[b : b + 1, :] = jnp.sum(jnp.transpose(sums[b]), axis=0, keepdims=True)


def psi_and_density(lists, basis_t, below, own, above):
    owned, columns = own.shape
    _, count, depth, points = basis_t.shape
    wide = min(columns, 512)
    grant = 2 * (9 * owned * wide + 2 * count * points * wide + 4 * count * depth * points)
    tile = pl.BlockSpec((owned, wide), lambda i, lists: (0, i))
    return pl.pallas_call(
        psi_kernel,
        out_shape=(
            jax.ShapeDtypeStruct((count, points, columns), jnp.bfloat16),
            jax.ShapeDtypeStruct((count, points), jnp.float32),
        ),
        grid_spec=pltpu.PrefetchScalarGridSpec(
            num_scalar_prefetch=1,
            grid=(columns // wide,),
            in_specs=[
                pl.BlockSpec((1, count, depth, points), lambda i, lists: (1, 0, 0, 0)),
                tile,
                tile,
                tile,
            ],
            out_specs=(
                pl.BlockSpec((count, points, wide), lambda i, lists: (0, 0, i)),
                pl.BlockSpec((count, points), lambda i, lists: (0, 0)),
            ),
            scratch_shapes=[
                pltpu.VMEM((3 * owned, wide), jnp.bfloat16),
                pltpu.VMEM((count, points, LANES), jnp.float32),
                pltpu.VMEM((count, points, depth), jnp.bfloat16),
            ],
        ),
        compiler_params=pltpu.CompilerParams(vmem_limit_bytes=grant + (6 << 20)),
        cost_estimate=pl.CostEstimate(
            flops=2 * count * points * depth * columns,
            bytes_accessed=8 * owned * columns,
            transcendentals=0,
        ),
        name="psi_and_density",
    )(lists, basis_t, below, own, above)


def potential_kernel(
    shape, layers, psi, dens, info, mine, hot, hot_t, weights, scale, shift, mw, aw, head,
    pot, near, psi_low, psi_high, relay,
    dens_buf, info_buf, rows_out, rows_buf, scaled_out, scaled_buf, sent, got,
    psi_sent, psi_got, psi_passed,
):
    n_grid, n_atom = shape
    n = n_grid * n_atom
    grid, atom = lax.axis_index("grid"), lax.axis_index("atom")
    me = grid * n_atom + atom

    def other(d):
        t = lax.rem(me + d, n)
        return (t // n_atom, lax.rem(t, n_atom))

    def to_all(source, held, k):
        @pl.loop(1, n)
        def _(d):
            pltpu.make_async_remote_copy(
                src_ref=source,
                dst_ref=held.at[me],
                send_sem=sent.at[k],
                recv_sem=got.at[k],
                device_id=other(d),
                device_id_type=MESH,
            ).start()

    def wait_all(held, sem, count):
        part = held.at[pl.ds(0, count)]
        pltpu.make_async_copy(part, part, sem).wait()

    meet_all(shape)
    halo = Halo(n_grid, layers + 2, psi, psi_low, psi_high, relay, psi_sent, psi_got, psi_passed)

    @pl.loop(1, n_atom)
    def _(d):
        to = lax.rem(atom + d, n_atom)
        pltpu.make_async_remote_copy(
            src_ref=dens.at[to],
            dst_ref=dens_buf.at[atom],
            send_sem=sent.at[0],
            recv_sem=got.at[0],
            device_id=(grid, to),
            device_id_type=MESH,
        ).start()

    to_all(info, info_buf, 1)
    halo.send(0)
    dens_buf[atom] = dens[atom]
    info_buf[me] = info[...]
    weight = to_columns(weights[...])[:, 0:1]

    wait_all(dens_buf, got.at[0], n_atom - 1)
    density = to_columns(2.0 * jnp.sum(dens_buf[...], axis=0))
    safe = jnp.where(density > 0.0, density, 1.0)
    radius = jnp.where(density > 0.0, jnp.exp(jnp.log(safe) * (1.0 / 3.0)), 0.0)[:, 0:1]
    hidden = jax.nn.silu(radius * scale[...] + shift[...])
    halves = hidden.shape[1] // LANES
    picks = []
    share = None
    for layer in range(layers):
        message = jax.nn.silu(
            jnp.dot(hidden.astype(jnp.bfloat16), mw[layer], preferred_element_type=jnp.float32)
        )
        weighted = (weight * message).astype(jnp.bfloat16)
        part = jnp.dot(hot_t[...], weighted, preferred_element_type=jnp.float32)
        rows_out[layer] = jnp.concatenate(
            [part[0:RUN, h * LANES : (h + 1) * LANES] for h in range(halves)], axis=0
        ).astype(jnp.bfloat16)
        to_all(rows_out.at[layer], rows_buf.at[layer], 2 + layer)
        halo.send(1 + layer)
        if layer == 0:
            halo.send(layers + 1)
        rows_buf[layer, me] = rows_out[layer]
        if layer == 0:
            wait_all(info_buf, got.at[1], n - 1)
            facts = info_buf[...].reshape(n * RUN, LANES)
            same = (facts[:, 0:1] == mine[...]).astype(jnp.float32)
            mass = jnp.sum(same * facts[:, LANES // 2 : LANES // 2 + 1], axis=0, keepdims=True)
            share = 1.0 / (1.0 + to_columns(mass)[:, 0:1])
            same = same.reshape(n, RUN, LANES)
            none = jnp.zeros_like(same)
            for h in range(halves):
                full = jnp.concatenate(
                    [same if k == h else none for k in range(halves)], axis=1
                ).reshape(n * RUN * halves, LANES)
                picks.append(jnp.transpose(full).astype(jnp.bfloat16))
        wait_all(rows_buf.at[layer], got.at[2 + layer], n - 1)
        halo.forward(layer)
        held = rows_buf[layer].reshape(n * RUN * halves, LANES)
        rows = jnp.concatenate(
            [jnp.dot(pick, held, preferred_element_type=jnp.float32) for pick in picks], axis=1
        )
        update = jax.nn.silu(
            jnp.dot(
                (rows * share).astype(jnp.bfloat16), aw[layer], preferred_element_type=jnp.float32
            )
        ).astype(jnp.bfloat16)
        picked = jnp.dot(hot[...], update, preferred_element_type=jnp.float32)
        hidden = hidden + message * picked
    score = jnp.sum(hidden * head[...], axis=1, keepdims=True)
    potential = radius * (1.0 + jnp.tanh(score))
    pot[...] = to_rows(potential)
    last = 2 + layers
    scaled_out[...] = to_rows(weight * potential)
    to_all(scaled_out, scaled_buf, last)
    scaled_buf[me] = scaled_out[...]
    wait_all(scaled_buf, got.at[last], n - 1)
    halo.forward(layers)
    halo.forward(layers + 1)
    for k in range(3):
        group = jnp.clip(grid - 1 + k, 0, n_grid - 1)
        near[k * n_atom : (k + 1) * n_atom] = scaled_buf[pl.ds(group * n_atom, n_atom)]
    wait_all(dens_buf, sent.at[0], n_atom - 1)
    wait_all(info_buf, sent.at[1], n - 1)
    for layer in range(layers):
        wait_all(rows_buf.at[layer], sent.at[2 + layer], n - 1)
    wait_all(scaled_buf, sent.at[last], n - 1)
    halo.finish()


def potential_of(shape, psi, dens, info, mine, hot, hot_t, weights, scale, shift, mw, aw, head):
    n_atom, batches, points = dens.shape
    n = shape[0] * shape[1]
    layers, features, _ = mw.shape
    packed = RUN * (features // LANES)
    anywhere = pl.BlockSpec(memory_space=pl.ANY)
    return pl.pallas_call(
        functools.partial(potential_kernel, shape, layers),
        out_shape=(
            jax.ShapeDtypeStruct((batches, points), jnp.float32),
            jax.ShapeDtypeStruct((3 * n_atom, batches, points), jnp.float32),
            jax.ShapeDtypeStruct(psi.shape, psi.dtype),
            jax.ShapeDtypeStruct(psi.shape, psi.dtype),
            jax.ShapeDtypeStruct((2, psi.shape[0] // 2, *psi.shape[1:]), psi.dtype),
        ),
        in_specs=[anywhere] + [VMEM] * 11,
        out_specs=(VMEM, VMEM, anywhere, anywhere, anywhere),
        scratch_shapes=[
            pltpu.VMEM((n_atom, batches, points), jnp.float32),
            pltpu.VMEM((n, RUN, LANES), jnp.float32),
            pltpu.VMEM((layers, packed, LANES), jnp.bfloat16),
            pltpu.VMEM((layers, n, packed, LANES), jnp.bfloat16),
            pltpu.VMEM((batches, points), jnp.float32),
            pltpu.VMEM((n, batches, points), jnp.float32),
            pltpu.SemaphoreType.DMA((3 + layers,)),
            pltpu.SemaphoreType.DMA((3 + layers,)),
        ]
        + halo_scratch(layers + 2),
        compiler_params=pltpu.CompilerParams(
            collective_id=0, has_side_effects=True, vmem_limit_bytes=24 << 20
        ),
        cost_estimate=pl.CostEstimate(
            flops=20_000_000_000, bytes_accessed=4_000_000, transcendentals=0
        ),
        name="potential_of",
    )(psi, dens, info, mine, hot, hot_t, weights, scale, shift, mw, aw, head)


def fock_kernel(lists, basis_t, near, low, mid, high, out, scaled):
    step = pl.program_id(0)
    groups, count, depth, points = basis_t.shape
    picks = lists.shape[1]
    width = depth // picks
    owned = out.shape[0] // width

    @pl.when(step == 0)
    def _():
        @pl.loop(0, groups)
        def _(k):
            @pl.loop(0, count)
            def _(b):
                scaled[k, b] = (
                    basis_t[k, b].astype(jnp.float32) * near[pl.ds(k * count + b, 1), :]
                ).astype(jnp.bfloat16)

    out[...] = jnp.zeros_like(out)
    for k, psi in enumerate((low, mid, high)):

        @pl.loop(0, count)
        def _(b, k=k, psi=psi):
            for j in range(picks):
                block = lists[k * count + b, j]

                @pl.when(jnp.logical_and(block >= 0, block < owned))
                def _():
                    at = pl.ds(pl.multiple_of(block * width, width), width)
                    out[at, :] += jnp.dot(
                        scaled[k, b, j * width : (j + 1) * width, :],
                        psi[b],
                        preferred_element_type=jnp.float32,
                    )


def fock_of(lists, basis_t, near, low, mid, high, owned):
    groups, count, depth, points = basis_t.shape
    columns = mid.shape[2]
    wide = min(columns, 512)
    tile = pl.BlockSpec((count, points, wide), lambda i, lists: (0, 0, i))
    grant = 2 * (9 * count * depth * points + 6 * count * points * wide + 4 * owned * wide)
    return pl.pallas_call(
        fock_kernel,
        out_shape=jax.ShapeDtypeStruct((owned, columns), jnp.float32),
        grid_spec=pltpu.PrefetchScalarGridSpec(
            num_scalar_prefetch=1,
            grid=(columns // wide,),
            in_specs=[
                pl.BlockSpec((groups, count, depth, points), lambda i, lists: (0, 0, 0, 0)),
                pl.BlockSpec((groups * count, points), lambda i, lists: (0, 0)),
                tile,
                tile,
                tile,
            ],
            out_specs=pl.BlockSpec((owned, wide), lambda i, lists: (0, i)),
            scratch_shapes=[pltpu.VMEM((groups, count, depth, points), jnp.bfloat16)],
        ),
        compiler_params=pltpu.CompilerParams(vmem_limit_bytes=grant + (4 << 20)),
        name="fock_of",
    )(lists, basis_t, near, low, mid, high)


def local(
    basis_values,
    block_lists,
    orbitals,
    point_weights,
    point_atoms,
    embed_scale,
    embed_shift,
    message_weight,
    atom_weight,
    head_weight,
):
    n_grid, n_atom = lax.axis_size("grid"), lax.axis_size("atom")
    own_rows = orbitals.shape[0]
    batches, points, depth = basis_values.shape
    width = depth // block_lists.shape[1]
    owned = own_rows // width
    shape = (n_grid, n_atom)
    first = lax.axis_index("grid") * owned
    names = jnp.pad(block_lists, ((0, 0), (0, LANES - block_lists.shape[1])))
    below, above, basis_t, names, _ = halo_of(
        shape, orbitals, jnp.swapaxes(basis_values, 1, 2), names
    )
    basis_t = basis_t.reshape(3, n_atom * batches, depth, points)
    lists = names[:, :, : block_lists.shape[1]].reshape(-1, block_lists.shape[1]) - first

    total = ATOM_DEV * n_atom
    lead = point_atoms[0]
    shifted = (point_atoms - lead + total // 2) % total - total // 2
    least = jnp.min(shifted)
    start = (lead + least) % total
    place = shifted - least
    lanes = jnp.arange(LANES, dtype=jnp.int32)
    onehot = place[:, None] == lanes[None, :]
    hot = onehot.astype(jnp.bfloat16)
    hot_t = (place[None, :] == lanes[:, None]).astype(jnp.bfloat16)
    mass = jnp.sum(jnp.where(onehot, point_weights[:, None], 0.0), axis=0)[:RUN]
    names = ((start + lanes) % total).astype(jnp.float32)
    mine = jnp.where(lanes < RUN, names, -1.0)[None, :]
    info = jnp.where(lanes[None, :] < LANES // 2, names[:RUN, None], mass[:, None])

    psi, dens = psi_and_density(block_lists - first + owned, basis_t, below, orbitals, above)
    potential, near, psi_low, psi_high, _ = potential_of(
        shape,
        psi,
        dens.reshape(n_atom, batches, points),
        info,
        mine,
        hot,
        hot_t,
        point_weights.reshape(batches, points),
        embed_scale[None, :],
        embed_shift[None, :],
        message_weight,
        atom_weight,
        head_weight[None, :],
    )
    fock = fock_of(
        lists, basis_t, near.reshape(-1, points), psi_low, psi, psi_high, own_rows
    )
    return (fock, potential.reshape(-1))


def solution(mesh):
    return jax.shard_map(
        local,
        mesh=mesh,
        in_specs=(
            P(("grid", "atom"), None, None),
            P("grid", None),
            P("grid", "atom"),
            P(("grid", "atom")),
            P(("grid", "atom")),
            P(),
            P(),
            P(),
            P(),
            P(),
        ),
        out_specs=(P("grid", "atom"), P(("grid", "atom"))),
        check_vma=False,
    )
```
